16 devices in a mesh: rep: 1, dp: 16 (over x, y, z, core).
Axes of the slice: x: 2, y: 2, z: 2, core: 2. Of those that a mesh axis runs over, the one named last changes fastest.
Arguments:
- g_w_gate: bfloat16 [16, 2, 1024, 3328], P(('rep', 'dp'))
- g_w_up: bfloat16 [16, 2, 1024, 3328], P(('rep', 'dp'))
- g_w_down: bfloat16 [16, 2, 3328, 1024], P(('rep', 'dp'))
- w_gate: bfloat16 [2, 1024, 3328], replicated
- w_up: bfloat16 [2, 1024, 3328], replicated
- w_down: bfloat16 [2, 3328, 1024], replicated
- m_w_gate: float32 [2, 1024, 3328], P(None, 'dp')
- m_w_up: float32 [2, 1024, 3328], P(None, 'dp')
- m_w_down: float32 [2, 3328, 1024], P(None, 'dp')
- v_w_gate: float32 [2, 1024, 3328], P(None, 'dp')
- v_w_up: float32 [2, 1024, 3328], P(None, 'dp')
- v_w_down: float32 [2, 3328, 1024], P(None, 'dp')
Outputs:
- output 1: bfloat16 [2, 1024, 3328], P('rep')
- output 2: bfloat16 [2, 1024, 3328], P('rep')
- output 3: bfloat16 [2, 3328, 1024], P('rep')
- output 4: float32 [2, 1024, 3328], P('rep', 'dp')
- output 5: float32 [2, 1024, 3328], P('rep', 'dp')
- output 6: float32 [2, 3328, 1024], P('rep', 'dp')
- output 7: float32 [2, 1024, 3328], P('rep', 'dp')
- output 8: float32 [2, 1024, 3328], P('rep', 'dp')
- output 9: float32 [2, 3328, 1024], P('rep', 'dp')
All inputs are finite; a program needn't handle non-finite values.
Results may differ from the reference program's by a relative error of at most 0.022.
Values are sent between devices in bfloat16 or wider.
A program may use at most 2 GiB of HBM per device.

```python
import jax
import jax.numpy as jnp
from jax import lax

DEVICES = 16
D = 1024
FF = 3328
LAYERS = 2
NAMES = ("w_gate", "w_up", "w_down")
SHAPES = {"w_gate": (LAYERS, D, FF), "w_up": (LAYERS, D, FF), "w_down": (LAYERS, FF, D)}


def setup_inputs(seed: int = 0, part: int = 0) -> dict:
    kz, *keys = jax.random.split(jax.random.key(seed), 1 + 5 * len(NAMES))
    loud = 2.0 ** jax.random.uniform(kz, (), jnp.float32, -1.0, 1.0)
    drawn = {}
    for name, key, both in zip(NAMES, keys[:3], keys[3:6], strict=True):
        own = jax.random.normal(jax.random.fold_in(key, part), (DEVICES, *SHAPES[name]), jnp.float32)
        shared = jax.random.normal(jax.random.fold_in(both, part), SHAPES[name], jnp.float32)
        drawn["g_" + name] = (loud * (0.7 * shared / DEVICES + 0.7 * own * DEVICES**-0.5)).astype(jnp.bfloat16)
    for name, key in zip(NAMES, keys[6:9], strict=True):
        drawn[name] = (jax.random.normal(key, SHAPES[name], jnp.float32) * SHAPES[name][1] ** -0.5).astype(jnp.bfloat16)
    for name, key in zip(NAMES, keys[9:12], strict=True):
        drawn["m_" + name] = loud * 0.5 * jax.random.normal(key, SHAPES[name], jnp.float32)
    for name, key in zip(NAMES, keys[12:15], strict=True):
        drawn["v_" + name] = loud * loud * jax.random.uniform(key, SHAPES[name], jnp.float32, 0.5, 1.5)
    return drawn


def adamw(w, m, v, g):
    m = 0.9 * m + 0.1 * g
    v = 0.95 * v + 0.05 * g * g
    step = m * lax.rsqrt(v + 1e-8) + 0.1 * w
    return (w - 0.02 * step).astype(jnp.bfloat16), m, v


def clipped(gradients, sum_of_squares, count):
    factor = jnp.minimum(1.0, 0.5 * lax.rsqrt(sum_of_squares / count + 1e-30))
    return [g * factor for g in gradients]


def reference(g_w_gate, g_w_up, g_w_down, w_gate, w_up, w_down, m_w_gate, m_w_up, m_w_down, v_w_gate, v_w_up, v_w_down):
    def total(terms):
        return lax.scan(lambda so_far, term: (so_far + term.astype(jnp.float32), None), jnp.zeros(terms.shape[1:], jnp.float32), terms)[0]

    gradients = [total(terms).astype(jnp.bfloat16).astype(jnp.float32) for terms in (g_w_gate, g_w_up, g_w_down)]
    gradients = clipped(gradients, sum(jnp.sum(g * g) for g in gradients), sum(g.size for g in gradients))
    new = [
        adamw(w.astype(jnp.float32), m, v, g)
        for w, m, v, g in zip((w_gate, w_up, w_down), (m_w_gate, m_w_up, m_w_down), (v_w_gate, v_w_up, v_w_down), gradients, strict=True)
    ]
    return tuple(one[which] for which in range(3) for one in new)
```

```python
import functools

import jax
import jax.numpy as jnp
from jax import lax
from jax.experimental import pallas as pl
from jax.experimental.pallas import tpu as pltpu
from jax.sharding import PartitionSpec as P

DEVICES = 16
LAYERS = 2
WINDOW = 12
BF16, F32 = jnp.bfloat16, jnp.float32
AXES = ((0, 1, 2), (1, 2, 0), (2, 0, 1))
UNITS = [(layer, w) for layer in range(LAYERS) for w in range(3)]


def gather_order():
    free, events, order = [0.0, 0.0, 0.0], [], []

    def send(now, layer, w, block):
        for bit in (0, 1, 2):
            if block >> bit:
                continue
            axis = AXES[w][2 - bit]
            free[axis] = max(free[axis], now) + 1.0
            events.append((free[axis], layer, w, block | 1 << bit))

    for i, (layer, w) in enumerate(UNITS):
        send(0.01 * i, layer, w, 0)
    while events:
        events.sort()
        now, layer, w, block = events.pop(0)
        order.append((layer, w, block))
        send(now + 0.1, layer, w, block)
    return order


def adamw(w, m, v, g):
    m = 0.9 * m + 0.1 * g
    v = 0.95 * v + 0.05 * g * g
    step = m * lax.rsqrt(v + 1e-8) + 0.1 * w
    return (w - 0.02 * step).astype(BF16), m, v


def tiles(rows, columns, body, init=None):
    def step(i, carry):
        for c in range(0, columns, 256):
            carry = body(pl.ds(pl.multiple_of(i * 16, 16), 16), pl.ds(c, 256), carry)
        return carry

    return lax.fori_loop(0, rows // 16, step, init)


def step_kernel(count, *refs):
    g, wt, m_in, v_in = (refs[i : i + 3] for i in (0, 3, 6, 9))
    out, m, v = (refs[i : i + 3] for i in (12, 15, 18))
    got2, got3, own_w = (refs[i : i + 3] for i in (21, 24, 27))
    squares, all_squares, send_sem, recv_sem, load_sem, in_sem, sum_send, sum_recv = refs[30:]
    rows = [ref.shape[2] // DEVICES for ref in g]
    columns = [ref.shape[3] for ref in g]

    me = lax.axis_index("dp")
    core = lax.rem(me, 2)
    bits = (me // 8, lax.rem(me // 4, 2), lax.rem(me // 2, 2))
    hop = [(1 - 2 * b) * s for b, s in zip(bits, (8, 4, 2), strict=True)]
    other = 1 - 2 * core

    def away(w, slot):
        return sum(hop[AXES[w][2 - bit]] for bit in range(3) if slot >> bit & 1)

    def block(w, index):
        return pl.ds(pl.multiple_of(index * rows[w], rows[w]), rows[w])

    def part(w, layer, unit):
        return out[w].at[layer, unit * rows[w] : (unit + 1) * rows[w]]

    def copy(w, layer, n, source, target, to):
        return pltpu.make_async_remote_copy(
            src_ref=source,
            dst_ref=target,
            send_sem=send_sem.at[layer * 3 + w, n],
            recv_sem=recv_sem.at[layer * 3 + w, n],
            device_id={"dp": me + to},
            device_id_type=pl.DeviceIdType.MESH,
        )

    def load(w, layer, slot):
        source = g[w].at[0, layer, block(w, me + away(w, slot))]
        return pltpu.make_async_copy(source, part(w, layer, slot + 4), load_sem.at[layer * 3 + w, slot])

    def swap(w, layer, slot):
        source = g[w].at[0, layer, block(w, me + other + away(w, slot))]
        return copy(w, layer, slot, source, part(w, layer, slot), other)

    def first(w, layer, slot):
        return copy(w, layer, 8 + slot - 4, part(w, layer, 4 + slot), part(w, layer, 8 + slot), hop[AXES[w][0]])

    def second(w, layer, slot):
        return copy(w, layer, 12 + slot - 2, part(w, layer, slot), got2[w].at[layer, slot - 2], hop[AXES[w][1]])

    def third(w, layer):
        return copy(w, layer, 14, part(w, layer, 1), got3[w].at[layer], hop[AXES[w][2]])

    early = [(w, layer, slot) for layer in range(LAYERS) for slot in (7, 6, 5, 4) for w in range(3)]
    late = [(w, layer, slot) for pair in ((3, 2), (1,), (0,)) for layer in range(LAYERS) for slot in pair for w in range(3)]
    for unit in early:
        load(*unit).start()

    barrier = pltpu.get_barrier_semaphore()
    for to in (other, *hop):
        pl.semaphore_signal(barrier, inc=1, device_id={"dp": me + to}, device_id_type=pl.DeviceIdType.MESH)
    pl.semaphore_wait(barrier, 4)

    swaps = [swap(*unit) for unit in early + late]
    for c in swaps[:WINDOW]:
        c.start()

    def total(w, sources, target):
        def tile(r, c, carry):
            acc = sources[0][r, c].astype(F32)
            for s in sources[1:]:
                acc += s[r, c].astype(F32)
            target[r, c] = acc.astype(BF16)
            return carry

        tiles(rows[w], columns[w], tile)

    for i, (w, layer, slot) in enumerate(early):
        load(w, layer, slot).wait()
        swaps[i].wait_recv()
        total(w, [part(w, layer, 4 + slot), part(w, layer, slot)], part(w, layer, 4 + slot))
        first(w, layer, slot).start()
        load(w, layer, slot - 4).start()
        if i + WINDOW < len(swaps):
            swaps[i + WINDOW].start()

    moments = [
        pltpu.make_async_copy(source[w].at[:, block(w, me)] if source is wt else source[w], target[w], in_sem.at[w, k])
        for w in range(3)
        for k, (source, target) in enumerate(((m_in, m), (v_in, v), (wt, own_w)))
    ]
    for c in moments:
        c.start()

    squares[...] = jnp.zeros_like(squares)
    for i, (w, layer, slot) in enumerate(late, len(early)):
        load(w, layer, slot).wait()
        swaps[i].wait_recv()
        first(w, layer, slot + 4).wait_recv()
        sources = [part(w, layer, slot + 4), part(w, layer, slot), part(w, layer, 12 + slot)]
        if slot < 2:
            second(w, layer, slot + 2).wait_recv()
            sources.append(got2[w].at[layer, slot])
        if slot == 0:
            third(w, layer).wait_recv()
            last = got3[w].at[layer]
            sources.append(last)

            def tile(r, c, carry, sources=sources, last=last):
                acc = sources[0][r, c].astype(F32)
                for s in sources[1:]:
                    acc += s[r, c].astype(F32)
                rounded = acc.astype(BF16)
                last[r, c] = rounded
                rounded = rounded.astype(F32)
                return carry + rounded * rounded

            squares[...] += tiles(rows[w], columns[w], tile, jnp.zeros((16, 256), F32))
        else:
            total(w, sources, part(w, layer, slot))
            (third(w, layer) if slot == 1 else second(w, layer, slot)).start()
        if i + WINDOW < len(swaps):
            swaps[i + WINDOW].start()

    for c in swaps:
        c.wait_send()
    for w, layer, slot in early:
        first(w, layer, slot).wait_send()
    for w, layer, slot in late:
        if slot:
            (third(w, layer) if slot == 1 else second(w, layer, slot)).wait_send()

    everyone = [
        pltpu.make_async_remote_copy(
            src_ref=all_squares.at[0],
            dst_ref=all_squares.at[k],
            send_sem=sum_send.at[k],
            recv_sem=sum_recv.at[k],
            device_id={"dp": lax.rem(me + k, DEVICES)},
            device_id_type=pl.DeviceIdType.MESH,
        )
        for k in range(1, DEVICES)
    ]
    s = squares[...]
    s = s[:8] + s[8:]
    all_squares[0] = s[:, :128] + s[:, 128:]
    for c in everyone:
        c.start()
    for c in moments:
        c.wait()
    for c in everyone:
        c.wait_recv()
    s = jnp.sum(jnp.sum(jnp.sum(all_squares[...], axis=0), axis=0, keepdims=True), axis=1, keepdims=True)
    factor = jnp.minimum(1.0, 0.5 * lax.rsqrt(s / count + 1e-30))

    def forward(w, layer, k, bit):
        where = out[w].at[layer, block(w, me + away(w, k))]
        return copy(w, layer, 7 + k if bit == 3 else (k | 1 << bit) - 1, where, where, other if bit == 3 else hop[AXES[w][2 - bit]])

    def arrived(w, layer, k):
        bit = k.bit_length() - 1
        return copy(w, layer, k - 1, out[w].at[layer, block(w, me)], out[w].at[layer, block(w, me + away(w, k))], hop[AXES[w][2 - bit]])

    sent = []

    def pass_on(w, layer, k):
        for bit in range(4):
            if not k >> bit or bit == 3:
                sent.append(forward(w, layer, k, bit))
                sent[-1].start()

    for layer, w in UNITS:

        def tile(r, c, carry, layer=layer, w=w):
            grad = got3[w][layer, r, c].astype(F32) * factor
            new, m[w][layer, r, c], v[w][layer, r, c] = adamw(own_w[w][layer, r, c].astype(F32), m[w][layer, r, c], v[w][layer, r, c], grad)
            own_w[w][layer, r, c] = new
            at = pl.ds(pl.multiple_of(me * rows[w] + r.start, 16), 16)
            out[w][layer, at, c] = new
            return carry

        tiles(rows[w], columns[w], tile)
        pass_on(w, layer, 0)
    for layer, w, k in gather_order():
        arrived(w, layer, k).wait_recv()
        pass_on(w, layer, k)
    for layer, w in UNITS:
        for k in range(8):
            where = out[w].at[layer, block(w, me + other + away(w, k))]
            copy(w, layer, 7 + k, where, where, other).wait_recv()
    for c in sent:
        c.wait_send()
    for c in everyone:
        c.wait_send()


def write_kernel(*refs):
    sem = refs[18]
    copies = [pltpu.make_async_copy(refs[i].at[layer], refs[9 + i].at[layer], sem.at[i, layer]) for i in range(9) for layer in range(LAYERS)]
    for c in copies:
        c.start()
    for c in copies:
        c.wait()


def solution(mesh):
    def step(*arrays):
        weights, moments = arrays[3:6], arrays[6:12]
        blocks = [one.shape for one in moments[:3]]
        new = [pltpu.VMEM(w.shape, BF16) for w in weights] + [pltpu.VMEM(one.shape, F32) for one in moments]
        hbm, vmem = pl.BlockSpec(memory_space=pl.ANY), pl.BlockSpec(memory_space=pltpu.VMEM)
        dma = pltpu.SemaphoreType.DMA
        count = float(sum(w.size for w in weights))
        new = pl.pallas_call(
            functools.partial(step_kernel, count),
            out_shape=new,
            in_specs=[hbm] * 12,
            out_specs=[vmem] * 9,
            scratch_shapes=[
                *(pltpu.VMEM((LAYERS, 2, *b[1:]), BF16) for b in blocks),
                *(pltpu.VMEM(b, BF16) for b in blocks),
                *(pltpu.VMEM(b, BF16) for b in blocks),
                pltpu.VMEM((16, 256), F32),
                pltpu.VMEM((DEVICES, 8, 128), F32),
                dma((6, 15)),
                dma((6, 15)),
                dma((6, 8)),
                dma((3, 3)),
                dma((DEVICES,)),
                dma((DEVICES,)),
            ],
            compiler_params=pltpu.CompilerParams(collective_id=0, has_side_effects=True, vmem_limit_bytes=12 * 2**20),
            name="step",
        )(*arrays)
        return tuple(
            pl.pallas_call(
                write_kernel,
                out_shape=[jax.ShapeDtypeStruct(one.shape, one.dtype) for one in new],
                in_specs=[hbm] * 9,
                out_specs=[hbm] * 9,
                scratch_shapes=[dma((9, LAYERS))],
                compiler_params=pltpu.CompilerParams(vmem_limit_bytes=2**20),
                name="write",
            )(*new)
        )

    all_of, cut = P(None, None, None), P(None, "dp", None)
    return jax.shard_map(
        step,
        mesh=mesh,
        in_specs=(P(("rep", "dp"), None, None, None),) * 3 + (all_of,) * 3 + (cut,) * 6,
        out_specs=(P("rep", None, None),) * 3 + (P("rep", "dp", None),) * 6,
        check_vma=False,
    )
```

```python
import functools

import jax
import jax.numpy as jnp
from jax import lax
from jax.experimental import pallas as pl
from jax.experimental.pallas import tpu as pltpu
from jax.sharding import PartitionSpec as P

DEVICES = 16
LAYERS = 2
WINDOW = 12
BF16, F32 = jnp.bfloat16, jnp.float32
AXES = ((0, 1, 2), (1, 2, 0), (2, 0, 1))
UNITS = [(layer, w) for layer in range(LAYERS) for w in range(3)]


def gather_order():
    free, events, order = [0.0, 0.0, 0.0], [], []

    def send(now, layer, w, block):
        for bit in (0, 1, 2):
            if block >> bit:
                continue
            axis = AXES[w][2 - bit]
            free[axis] = max(free[axis], now) + 1.0
            events.append((free[axis], layer, w, block | 1 << bit))

    for i, (layer, w) in enumerate(UNITS):
        send(0.01 * i, layer, w, 0)
    while events:
        events.sort()
        now, layer, w, block = events.pop(0)
        order.append((layer, w, block))
        send(now + 0.1, layer, w, block)
    return order


def adamw(w, m, v, g):
    m = 0.9 * m + 0.1 * g
    v = 0.95 * v + 0.05 * g * g
    step = m * lax.rsqrt(v + 1e-8) + 0.1 * w
    return (w - 0.02 * step).astype(BF16), m, v


def tiles(rows, columns, body, init=None):
    def step(i, carry):
        for c in range(0, columns, 256):
            carry = body(pl.ds(pl.multiple_of(i * 16, 16), 16), pl.ds(c, 256), carry)
        return carry

    return lax.fori_loop(0, rows // 16, step, init)


def step_kernel(count, *refs):
    g, wt, m_in, v_in = (refs[i : i + 3] for i in (0, 3, 6, 9))
    out, m, v = (refs[i : i + 3] for i in (12, 15, 18))
    wide, tall, squares, all_squares, send_sem, recv_sem, load_sem, in_sem, tile_sem, sum_send, sum_recv, free_sem = refs[21:]
    rows = [ref.shape[2] // DEVICES for ref in g]
    columns = [ref.shape[3] for ref in g]

    me = lax.axis_index("dp")
    core = lax.rem(me, 2)
    bits = (me // 8, lax.rem(me // 4, 2), lax.rem(me // 2, 2))
    hop = [(1 - 2 * b) * s for b, s in zip(bits, (8, 4, 2), strict=True)]
    other = 1 - 2 * core

    def away(w, slot):
        return sum(hop[AXES[w][2 - bit]] for bit in range(3) if slot >> bit & 1)

    def block(w, index):
        return pl.ds(pl.multiple_of(index * rows[w], rows[w]), rows[w])

    def part(w, layer, unit):
        return out[w].at[layer, unit * rows[w] : (unit + 1) * rows[w]]

    def copy(w, layer, n, source, target, to):
        return pltpu.make_async_remote_copy(
            src_ref=source,
            dst_ref=target,
            send_sem=send_sem.at[layer * 3 + w, n],
            recv_sem=recv_sem.at[layer * 3 + w, n],
            device_id={"dp": me + to},
            device_id_type=pl.DeviceIdType.MESH,
        )

    def load(w, layer, slot):
        source = g[w].at[0, layer, block(w, me + away(w, slot))]
        return pltpu.make_async_copy(source, part(w, layer, slot + 4), load_sem.at[layer * 3 + w, slot])

    def swap(w, layer, slot):
        source = g[w].at[0, layer, block(w, me + other + away(w, slot))]
        return copy(w, layer, slot, source, part(w, layer, slot), other)

    def first(w, layer, slot):
        return copy(w, layer, 8 + slot - 4, part(w, layer, 4 + slot), part(w, layer, 8 + slot), hop[AXES[w][0]])

    def second(w, layer, slot):
        return copy(w, layer, 12 + slot - 2, part(w, layer, slot), part(w, layer, 8 + slot), hop[AXES[w][1]])

    def third(w, layer):
        return copy(w, layer, 14, part(w, layer, 1), part(w, layer, 9), hop[AXES[w][2]])

    early = [(w, layer, slot) for layer in range(LAYERS) for slot in (7, 6, 5, 4) for w in range(3)]
    late = [(w, layer, slot) for pair in ((3, 2), (1,), (0,)) for layer in range(LAYERS) for slot in pair for w in range(3)]
    for unit in early:
        load(*unit).start()

    barrier = pltpu.get_barrier_semaphore()
    for to in (other, *hop):
        pl.semaphore_signal(barrier, inc=1, device_id={"dp": me + to}, device_id_type=pl.DeviceIdType.MESH)
    pl.semaphore_wait(barrier, 4)

    swaps = [swap(*unit) for unit in early + late]
    for c in swaps[:WINDOW]:
        c.start()

    def total(w, sources, target):
        def tile(r, c, carry):
            acc = sources[0][r, c].astype(F32)
            for s in sources[1:]:
                acc += s[r, c].astype(F32)
            target[r, c] = acc.astype(BF16)
            return carry

        tiles(rows[w], columns[w], tile)

    for i, (w, layer, slot) in enumerate(early):
        load(w, layer, slot).wait()
        swaps[i].wait_recv()
        total(w, [part(w, layer, 4 + slot), part(w, layer, slot)], part(w, layer, 4 + slot))
        first(w, layer, slot).start()
        load(w, layer, slot - 4).start()
        if i + WINDOW < len(swaps):
            swaps[i + WINDOW].start()

    loads = [pltpu.make_async_copy(m_in[w], m[w], in_sem.at[w, 0]) for w in range(3)]
    for c in loads:
        c.start()

    def tile_load(w, layer, i, slot):
        source = v_in[w].at[layer, pl.ds(pl.multiple_of(i * 16, 16), 16)]
        return pltpu.make_async_copy(source, (tall if w == 2 else wide).at[slot], tile_sem.at[int(w == 2), slot])

    for i in range(4):
        tile_load(0, 0, i, i).start()
        tile_load(2, 0, i, i).start()

    squares[...] = jnp.zeros_like(squares)
    freed = set()
    for i, (w, layer, slot) in enumerate(late, len(early)):
        if layer not in freed:
            freed.add(layer)
            for x in range(3):
                for sent_slot in (7, 6, 5):
                    first(x, layer, sent_slot).wait_send()
                for axis in (1, 2):
                    to = {"dp": me + hop[AXES[x][axis]]}
                    pl.semaphore_signal(free_sem.at[layer * 3 + x, axis - 1], inc=1, device_id=to, device_id_type=pl.DeviceIdType.MESH)
        load(w, layer, slot).wait()
        swaps[i].wait_recv()
        first(w, layer, slot + 4).wait_recv()
        sources = [part(w, layer, slot + 4), part(w, layer, slot), part(w, layer, 12 + slot)]
        if slot < 2:
            second(w, layer, slot + 2).wait_recv()
            sources.append(part(w, layer, 10 + slot))
        if slot == 0:
            third(w, layer).wait_recv()
            sources.append(part(w, layer, 9))

            def tile(r, c, carry, sources=sources, w=w, layer=layer):
                acc = sources[0][r, c].astype(F32)
                for s in sources[1:]:
                    acc += s[r, c].astype(F32)
                rounded = acc.astype(BF16).astype(F32)
                v[w][layer, r, c] = rounded
                return carry + rounded * rounded

            squares[...] += tiles(rows[w], columns[w], tile, jnp.zeros((16, 256), F32))
        else:
            total(w, sources, part(w, layer, slot))
            if slot in (3, 1):
                pl.semaphore_wait(free_sem.at[layer * 3 + w, int(slot == 1)], 1)
            (third(w, layer) if slot == 1 else second(w, layer, slot)).start()
        if i + WINDOW < len(swaps):
            swaps[i + WINDOW].start()

    for c in swaps:
        c.wait_send()
    for layer, w in UNITS:
        first(w, layer, 4).wait_send()
    for w, layer, slot in late:
        if slot:
            (third(w, layer) if slot == 1 else second(w, layer, slot)).wait_send()

    everyone = [
        pltpu.make_async_remote_copy(
            src_ref=all_squares.at[0],
            dst_ref=all_squares.at[k],
            send_sem=sum_send.at[k],
            recv_sem=sum_recv.at[k],
            device_id={"dp": lax.rem(me + k, DEVICES)},
            device_id_type=pl.DeviceIdType.MESH,
        )
        for k in range(1, DEVICES)
    ]
    s = squares[...]
    s = s[:8] + s[8:]
    all_squares[0] = s[:, :128] + s[:, 128:]
    for c in everyone:
        c.start()
    loads += [pltpu.make_async_copy(wt[w].at[:, block(w, me)], out[w].at[:, block(w, me)], in_sem.at[w, 1]) for w in range(3)]
    for c in loads[3:]:
        c.start()
    for c in loads:
        c.wait()
    for c in everyone:
        c.wait_recv()
    s = jnp.sum(jnp.sum(jnp.sum(all_squares[...], axis=0), axis=0, keepdims=True), axis=1, keepdims=True)
    factor = jnp.minimum(1.0, 0.5 * lax.rsqrt(s / count + 1e-30))

    def forward(w, layer, k, bit):
        where = out[w].at[layer, block(w, me + away(w, k))]
        return copy(w, layer, 7 + k if bit == 3 else (k | 1 << bit) - 1, where, where, other if bit == 3 else hop[AXES[w][2 - bit]])

    def arrived(w, layer, k):
        bit = k.bit_length() - 1
        return copy(w, layer, k - 1, out[w].at[layer, block(w, me)], out[w].at[layer, block(w, me + away(w, k))], hop[AXES[w][2 - bit]])

    sent = []

    def pass_on(w, layer, k):
        for bit in range(4):
            if not k >> bit or bit == 3:
                sent.append(forward(w, layer, k, bit))
                sent[-1].start()

    def advance(w, layer, i):
        slot = i if w < 2 else lax.rem(layer * (rows[w] // 16) + i, 4)
        tile_load(w, layer, i, slot).wait()
        r = pl.ds(pl.multiple_of(i * 16, 16), 16)
        at = pl.ds(pl.multiple_of(me * rows[w] + i * 16, 16), 16)
        for column in range(0, columns[w], 256):
            c = pl.ds(column, 256)
            old = (tall if w == 2 else wide)[slot, :, c]
            new, m[w][layer, r, c], v[w][layer, r, c] = adamw(
                out[w][layer, at, c].astype(F32), m[w][layer, r, c], old, v[w][layer, r, c] * factor
            )
            out[w][layer, at, c] = new
        if w == 0:
            tile_load(1, layer, i, slot).start()
        elif w == 1 and layer + 1 < LAYERS:
            tile_load(0, layer + 1, i, slot).start()
        elif w == 2:
            ahead = i + 4

            @pl.when(ahead < rows[w] // 16)
            def _():
                tile_load(w, layer, ahead, slot).start()

            if layer + 1 < LAYERS:

                @pl.when(ahead >= rows[w] // 16)
                def _():
                    tile_load(w, layer + 1, ahead - rows[w] // 16, slot).start()

    for layer, w in UNITS:
        lax.fori_loop(0, rows[w] // 16, lambda i, _, w=w, layer=layer: advance(w, layer, i), None)
        pass_on(w, layer, 0)
    for layer, w, k in gather_order():
        arrived(w, layer, k).wait_recv()
        pass_on(w, layer, k)
    for layer, w in UNITS:
        for k in range(8):
            where = out[w].at[layer, block(w, me + other + away(w, k))]
            copy(w, layer, 7 + k, where, where, other).wait_recv()
    for c in sent:
        c.wait_send()
    for c in everyone:
        c.wait_send()


def write_kernel(*refs):
    sem = refs[18]
    copies = [pltpu.make_async_copy(refs[i].at[layer], refs[9 + i].at[layer], sem.at[i, layer]) for i in range(9) for layer in range(LAYERS)]
    for c in copies:
        c.start()
    for c in copies:
        c.wait()


def solution(mesh):
    def step(*arrays):
        weights, moments = arrays[3:6], arrays[6:12]
        blocks = [one.shape for one in moments[:3]]
        new = [pltpu.VMEM(w.shape, BF16) for w in weights] + [pltpu.VMEM(one.shape, F32) for one in moments]
        hbm, vmem = pl.BlockSpec(memory_space=pltpu.HBM), pl.BlockSpec(memory_space=pltpu.VMEM)
        dma = pltpu.SemaphoreType.DMA
        count = float(sum(w.size for w in weights))
        new = pl.pallas_call(
            functools.partial(step_kernel, count),
            out_shape=new,
            in_specs=[hbm] * 12,
            out_specs=[vmem] * 9,
            scratch_shapes=[
                pltpu.VMEM((4, 16, blocks[0][2]), F32),
                pltpu.VMEM((4, 16, blocks[2][2]), F32),
                pltpu.VMEM((16, 256), F32),
                pltpu.VMEM((DEVICES, 8, 128), F32),
                dma((6, 15)),
                dma((6, 15)),
                dma((6, 8)),
                dma((3, 2)),
                dma((2, 4)),
                dma((DEVICES,)),
                dma((DEVICES,)),
                pltpu.SemaphoreType.REGULAR((6, 2)),
            ],
            compiler_params=pltpu.CompilerParams(collective_id=0, has_side_effects=True, vmem_limit_bytes=5 * 2**18),
            name="step",
        )(*(pltpu.with_memory_space_constraint(a, pltpu.HBM) for a in arrays))
        return tuple(
            pl.pallas_call(
                write_kernel,
                out_shape=[jax.ShapeDtypeStruct(one.shape, one.dtype) for one in new],
                in_specs=[vmem] * 9,
                out_specs=[hbm] * 9,
                scratch_shapes=[dma((9, LAYERS))],
                compiler_params=pltpu.CompilerParams(vmem_limit_bytes=2**18),
                name="write",
            )(*(pltpu.with_memory_space_constraint(a, pltpu.VMEM) for a in new))
        )

    all_of, cut = P(None, None, None), P(None, "dp", None)
    return jax.shard_map(
        step,
        mesh=mesh,
        in_specs=(P(("rep", "dp"), None, None, None),) * 3 + (all_of,) * 3 + (cut,) * 6,
        out_specs=(P("rep", None, None),) * 3 + (P("rep", "dp", None),) * 6,
        check_vma=False,
    )
```

```python
import functools

import jax
import jax.numpy as jnp
from jax import lax
from jax.experimental import pallas as pl
from jax.experimental.pallas import tpu as pltpu
from jax.sharding import PartitionSpec as P

DEVICES = 16
LAYERS = 2
WINDOW = 12
BF16, F32 = jnp.bfloat16, jnp.float32
AXES = ((0, 1, 2), (1, 2, 0), (2, 0, 1))
WIDTH = 1664
PIECES = 4
UNITS = [(layer, w) for layer in range(LAYERS) for w in range(3)]


def gather_order():
    free, events, order = [0.0, 0.0, 0.0], [], []

    def send(now, layer, w, block):
        for bit in (0, 1, 2):
            if block >> bit:
                continue
            axis = AXES[w][2 - bit]
            free[axis] = max(free[axis], now) + 1.0
            events.append((free[axis], layer, w, block | 1 << bit))

    for i, (layer, w) in enumerate(UNITS):
        send(0.01 * i, layer, w, 0)
    while events:
        events.sort()
        now, layer, w, block = events.pop(0)
        order.append((layer, w, block))
        send(now + 0.1, layer, w, block)
    return order


def adamw(w, m, v, g):
    m = 0.9 * m + 0.1 * g
    v = 0.95 * v + 0.05 * g * g
    step = m * lax.rsqrt(v + 1e-8) + 0.1 * w
    return (w - 0.02 * step).astype(BF16), m, v


def tiles(rows, columns, body):
    width = WIDTH if columns % WIDTH == 0 else columns

    def step(i, _):
        for c in range(0, columns, width):
            body(pl.ds(pl.multiple_of(i * 16, 16), 16), pl.ds(c, width))

    lax.fori_loop(0, rows // 16, step, None)


def each(n, body):
    lax.fori_loop(0, n, lambda p, _: body(p), None)


def step_kernel(count, *refs):
    g, wt, m_in, v_in = (refs[i : i + 3] for i in (0, 3, 6, 9))
    out, m, v = (refs[i : i + 3] for i in (12, 15, 18))
    wide, tall, squares, all_squares, send_sem, recv_sem, load_sem, in_sem, tile_sem, sum_send, sum_recv, free_sem, cut_send, cut_recv = refs[21:]
    rows = [ref.shape[2] // DEVICES for ref in g]
    columns = [ref.shape[3] for ref in g]

    me = lax.axis_index("dp")
    core = lax.rem(me, 2)
    bits = (me // 8, lax.rem(me // 4, 2), lax.rem(me // 2, 2))
    hop = [(1 - 2 * b) * s for b, s in zip(bits, (8, 4, 2), strict=True)]
    other = 1 - 2 * core

    def away(w, slot):
        return sum(hop[AXES[w][2 - bit]] for bit in range(3) if slot >> bit & 1)

    def block(w, index):
        return pl.ds(pl.multiple_of(index * rows[w], rows[w]), rows[w])

    def part(w, layer, unit):
        return out[w].at[layer, unit * rows[w] : (unit + 1) * rows[w]]

    def copy(w, layer, n, source, target, to):
        return pltpu.make_async_remote_copy(
            src_ref=source,
            dst_ref=target,
            send_sem=send_sem.at[layer * 3 + w, n],
            recv_sem=recv_sem.at[layer * 3 + w, n],
            device_id={"dp": me + to},
            device_id_type=pl.DeviceIdType.MESH,
        )

    def piece(w, ref, p):
        return ref.at[:, pl.ds(pl.multiple_of(p * 256, 256), 256)] if w == 2 else ref.at[pl.ds(pl.multiple_of(p * 16, 16), 16)]

    def cut_copy(kind, n, p, source, target, to, w=None):
        w = n if w is None else w
        return pltpu.make_async_remote_copy(
            src_ref=piece(w, source, p),
            dst_ref=piece(w, target, p),
            send_sem=cut_send.at[kind, n, p],
            recv_sem=cut_recv.at[kind, n, p],
            device_id={"dp": me + to},
            device_id_type=pl.DeviceIdType.MESH,
        )

    def load(w, layer, slot):
        source = g[w].at[0, layer, block(w, me + away(w, slot))]
        return pltpu.make_async_copy(source, part(w, layer, slot + 4), load_sem.at[layer * 3 + w, slot])

    def swap(w, layer, slot):
        source = g[w].at[0, layer, block(w, me + other + away(w, slot))]
        if (layer, slot) == (0, 7):
            return PIECES, lambda p: cut_copy(0, w, p, source, part(w, layer, slot), other)
        return 1, lambda p: copy(w, layer, slot, source, part(w, layer, slot), other)

    def first(w, layer, slot):
        source, target, to = part(w, layer, 4 + slot), part(w, layer, 8 + slot), hop[AXES[w][0]]
        if (layer, slot) == (0, 7):
            return PIECES, lambda p: cut_copy(1, w, p, source, target, to)
        return 1, lambda p: copy(w, layer, 8 + slot - 4, source, target, to)

    def second(w, layer, slot):
        return copy(w, layer, 12 + slot - 2, part(w, layer, slot), part(w, layer, 8 + slot), hop[AXES[w][1]])

    def third(w, layer):
        source, target, to = part(w, layer, 1), part(w, layer, 9), hop[AXES[w][2]]
        if layer == LAYERS - 1:
            return PIECES, lambda p: cut_copy(2, w, p, source, target, to)
        return 1, lambda p: copy(w, layer, 14, source, target, to)

    early = [(w, layer, slot) for layer in range(LAYERS) for slot in (7, 6, 5, 4) for w in range(3)]
    late = [(w, layer, slot) for pair in ((3, 2), (1,), (0,)) for layer in range(LAYERS) for slot in pair for w in range(3)]
    for unit in early:
        load(*unit).start()

    barrier = pltpu.get_barrier_semaphore()
    for to in (other, *hop):
        pl.semaphore_signal(barrier, inc=1, device_id={"dp": me + to}, device_id_type=pl.DeviceIdType.MESH)
    pl.semaphore_wait(barrier, 4)

    swaps = [swap(*unit) for unit in early + late]
    for p in range(PIECES):
        for w in range(3):
            swaps[w][1](p).start()
    for _, c in swaps[3:WINDOW]:
        c(0).start()

    def done(copies, side):
        n, c = copies
        if n == 1:
            getattr(c(0), side)()
        else:
            each(n, lambda p: getattr(c(p), side)())

    def add_up(sources, r, c):
        acc = sources[0][r, c].astype(F32)
        for s in sources[1:]:
            acc += s[r, c].astype(F32)
        return acc

    def total(sources, target):
        def tile(r, c):
            target[r, c] = add_up(sources, r, c).astype(BF16)

        tiles(*target.shape, tile)

    def join(w, layer, slot, p, swap_copy, first_copy):
        swap_copy.wait_recv()
        mine, theirs = part(w, layer, 4 + slot), part(w, layer, slot)
        if p is not None:
            mine, theirs = piece(w, mine, p), piece(w, theirs, p)
        total([mine, theirs], mine)
        first_copy.start()

    for w in range(3):
        load(w, 0, 7).wait()

    @functools.partial(each, PIECES)
    def _(p):
        for w in range(3):
            join(w, 0, 7, p, swaps[w][1](p), first(w, 0, 7)[1](p))

    for i, (w, layer, slot) in enumerate(early):
        if i >= 3:
            load(w, layer, slot).wait()
            join(w, layer, slot, None, swaps[i][1](0), first(w, layer, slot)[1](0))
        load(w, layer, slot - 4).start()
        if i + WINDOW < len(swaps):
            swaps[i + WINDOW][1](0).start()

    loads = [pltpu.make_async_copy(m_in[w], m[w], in_sem.at[w, 0]) for w in range(3)]
    for c in loads:
        c.start()

    def tile_load(w, layer, i, slot):
        source = v_in[w].at[layer, pl.ds(pl.multiple_of(i * 16, 16), 16)]
        return pltpu.make_async_copy(source, (tall if w == 2 else wide).at[slot], tile_sem.at[int(w == 2), slot])

    for i in range(4):
        tile_load(0, 0, i, i).start()
        tile_load(2, 0, i, i).start()

    squares[...] = jnp.zeros_like(squares)
    freed = set()
    for i, (w, layer, slot) in enumerate(late, len(early)):
        if layer not in freed:
            freed.add(layer)
            for x in range(3):
                for sent_slot in (7, 6, 5):
                    done(first(x, layer, sent_slot), "wait_send")
                for axis in (1, 2):
                    to = {"dp": me + hop[AXES[x][axis]]}
                    pl.semaphore_signal(free_sem.at[layer * 3 + x, axis - 1], inc=1, device_id=to, device_id_type=pl.DeviceIdType.MESH)
        load(w, layer, slot).wait()
        done(swaps[i], "wait_recv")
        done(first(w, layer, slot + 4), "wait_recv")
        sources = [part(w, layer, slot + 4), part(w, layer, slot), part(w, layer, 12 + slot)]
        if slot < 2:
            second(w, layer, slot + 2).wait_recv()
            sources.append(part(w, layer, 10 + slot))
        if slot == 0:

            def tile(r, c, sources=sources, w=w, layer=layer):
                v[w][layer, r, c] = add_up(sources, r, c)

            tiles(rows[w], columns[w], tile)
        elif slot == 1:
            pl.semaphore_wait(free_sem.at[layer * 3 + w, 1], 1)
            n, c = third(w, layer)
            target = part(w, layer, slot)
            if n == 1:
                total(sources, target)
                c(0).start()
            else:

                @functools.partial(each, n)
                def _(p, w=w, c=c, sources=sources, target=target):
                    total([piece(w, ref, p) for ref in sources], piece(w, target, p))
                    c(p).start()

        else:
            total(sources, part(w, layer, slot))
            if slot == 3:
                pl.semaphore_wait(free_sem.at[layer * 3 + w, 0], 1)
            second(w, layer, slot).start()
        if i + WINDOW < len(swaps):
            swaps[i + WINDOW][1](0).start()

    def finish(w, last, grad):
        def tile(r, c):
            rounded = (grad[r, c] + last[r, c].astype(F32)).astype(BF16).astype(F32)
            grad[r, c] = rounded
            squares[:, : c.size] += rounded * rounded

        tiles(*last.shape, tile)

    squares[...] = jnp.zeros_like(squares)
    for w in range(3):
        done(third(w, 0), "wait_recv")
        finish(w, part(w, 0, 9), v[w].at[0])

    @functools.partial(each, PIECES)
    def _(p):
        for w in range(3):
            third(w, 1)[1](p).wait_recv()
            finish(w, piece(w, part(w, 1, 9), p), piece(w, v[w].at[1], p))

    for copies in swaps:
        done(copies, "wait_send")
    for layer, w in UNITS:
        done(first(w, layer, 4), "wait_send")
        for slot in (3, 2):
            second(w, layer, slot).wait_send()
        done(third(w, layer), "wait_send")

    everyone = [
        pltpu.make_async_remote_copy(
            src_ref=all_squares.at[0],
            dst_ref=all_squares.at[k],
            send_sem=sum_send.at[k],
            recv_sem=sum_recv.at[k],
            device_id={"dp": lax.rem(me + k, DEVICES)},
            device_id_type=pl.DeviceIdType.MESH,
        )
        for k in range(1, DEVICES)
    ]
    s = squares[:8] + squares[8:]
    all_squares[0] = sum(s[:, c : c + 128] for c in range(0, WIDTH, 128))
    for c in everyone:
        c.start()
    loads += [pltpu.make_async_copy(wt[w].at[:, block(w, me)], out[w].at[:, block(w, me)], in_sem.at[w, 1]) for w in range(3)]
    for c in loads[3:]:
        c.start()
    for c in loads:
        c.wait()
    for c in everyone:
        c.wait_recv()
    s = jnp.sum(jnp.sum(jnp.sum(all_squares[...], axis=0), axis=0, keepdims=True), axis=1, keepdims=True)
    factor = jnp.minimum(1.0, 0.5 * lax.rsqrt(s / count + 1e-30))

    def forward(w, layer, k, bit):
        where = out[w].at[layer, block(w, me + away(w, k))]
        return copy(w, layer, 7 + k if bit == 3 else (k | 1 << bit) - 1, where, where, other if bit == 3 else hop[AXES[w][2 - bit]])

    def forward_cut(w, layer, k, bit, p):
        where = out[w].at[layer, block(w, me + away(w, k))]
        to = other if bit == 3 else hop[AXES[w][2 - bit]]
        if k:
            return cut_copy(3 + (bit == 3), w, p, where, where, to)
        return cut_copy(5, bit, p, where, where, to, 0)

    def arrived_cut(w, layer, k, p):
        source, target = out[w].at[layer, block(w, me)], out[w].at[layer, block(w, me + away(w, k))]
        kind, n = (5, k.bit_length() - 1) if layer == 0 else (3, w)
        return cut_copy(kind, n, p, source, target, hop[AXES[w][3 - k.bit_length()]], w)

    def arrived(w, layer, k):
        bit = k.bit_length() - 1
        return copy(w, layer, k - 1, out[w].at[layer, block(w, me)], out[w].at[layer, block(w, me + away(w, k))], hop[AXES[w][2 - bit]])

    sent = []

    def pass_on(w, layer, k):
        for bit in range(4):
            if not k >> bit or bit == 3:
                sent.append(forward(w, layer, k, bit))
                sent[-1].start()

    def advance(w, layer, i):
        slot = i if w < 2 else lax.rem(layer * (rows[w] // 16) + i, 4)
        tile_load(w, layer, i, slot).wait()
        r = pl.ds(pl.multiple_of(i * 16, 16), 16)
        at = pl.ds(pl.multiple_of(me * rows[w] + i * 16, 16), 16)
        for column in range(0, columns[w], 256):
            c = pl.ds(column, 256)
            old = (tall if w == 2 else wide)[slot, :, c]
            new, m[w][layer, r, c], v[w][layer, r, c] = adamw(
                out[w][layer, at, c].astype(F32), m[w][layer, r, c], old, v[w][layer, r, c] * factor
            )
            out[w][layer, at, c] = new
        if w == 0:
            tile_load(1, layer, i, slot).start()
        elif w == 1 and layer + 1 < LAYERS:
            tile_load(0, layer + 1, i, slot).start()
        elif w == 2:
            ahead = i + 4

            @pl.when(ahead < rows[w] // 16)
            def _():
                tile_load(w, layer, ahead, slot).start()

            if layer + 1 < LAYERS:

                @pl.when(ahead >= rows[w] // 16)
                def _():
                    tile_load(w, layer + 1, ahead - rows[w] // 16, slot).start()

    for layer, w in UNITS:
        if (layer, w) == (0, 0):

            @functools.partial(each, PIECES)
            def _(p):
                advance(0, 0, p)
                for bit in range(3):
                    forward_cut(0, 0, 0, bit, p).start()

            sent.append(forward(w, layer, 0, 3))
            sent[-1].start()
        else:
            lax.fori_loop(0, rows[w] // 16, lambda i, _, w=w, layer=layer: advance(w, layer, i), None)
            pass_on(w, layer, 0)
    order = gather_order()
    last = [(LAYERS - 1, w, 7) for w in range(3)]
    assert sorted(order[-3:]) == last
    for layer, w, k in order[:-3]:
        if (layer, w) == (0, 0) and k & k - 1 == 0:
            each(PIECES, lambda p, k=k: arrived_cut(0, 0, k, p).wait_recv())
        else:
            arrived(w, layer, k).wait_recv()
        if (layer, k) == (LAYERS - 1, 3):
            each(PIECES, lambda p, w=w: forward_cut(w, 1, 3, 2, p).start())
            sent.append(forward(w, layer, k, 3))
            sent[-1].start()
        else:
            pass_on(w, layer, k)

    @functools.partial(each, PIECES)
    def _(p):
        for w in range(3):
            arrived_cut(w, 1, 7, p).wait_recv()
            forward_cut(w, 1, 7, 3, p).start()

    for layer, w in UNITS:
        for k in range(8):
            where = out[w].at[layer, block(w, me + other + away(w, k))]
            if (layer, w, k) in last:
                each(PIECES, lambda p, w=w, where=where: cut_copy(4, w, p, where, where, other).wait_recv())
            else:
                copy(w, layer, 7 + k, where, where, other).wait_recv()
    for c in sent:
        c.wait_send()

    @functools.partial(each, PIECES)
    def _(p):
        for n in range(3):
            forward_cut(0, 0, 0, n, p).wait_send()
            forward_cut(n, 1, 3, 2, p).wait_send()
            forward_cut(n, 1, 7, 3, p).wait_send()

    for c in everyone:
        c.wait_send()


def write_kernel(*refs):
    sem = refs[18]
    copies = [pltpu.make_async_copy(refs[i].at[layer], refs[9 + i].at[layer], sem.at[i, layer]) for i in range(9) for layer in range(LAYERS)]
    for c in copies:
        c.start()
    for c in copies:
        c.wait()


def solution(mesh):
    def step(*arrays):
        weights, moments = arrays[3:6], arrays[6:12]
        blocks = [one.shape for one in moments[:3]]
        new = [pltpu.VMEM(w.shape, BF16) for w in weights] + [pltpu.VMEM(one.shape, F32) for one in moments]
        hbm, vmem = pl.BlockSpec(memory_space=pltpu.HBM), pl.BlockSpec(memory_space=pltpu.VMEM)
        dma = pltpu.SemaphoreType.DMA
        count = float(sum(w.size for w in weights))
        new = pl.pallas_call(
            functools.partial(step_kernel, count),
            out_shape=new,
            in_specs=[hbm] * 12,
            out_specs=[vmem] * 9,
            scratch_shapes=[
                pltpu.VMEM((4, 16, blocks[0][2]), F32),
                pltpu.VMEM((4, 16, blocks[2][2]), F32),
                pltpu.VMEM((16, WIDTH), F32),
                pltpu.VMEM((DEVICES, 8, 128), F32),
                dma((6, 15)),
                dma((6, 15)),
                dma((6, 8)),
                dma((3, 2)),
                dma((2, 4)),
                dma((DEVICES,)),
                dma((DEVICES,)),
                pltpu.SemaphoreType.REGULAR((6, 2)),
                dma((6, 3, PIECES)),
                dma((6, 3, PIECES)),
            ],
            compiler_params=pltpu.CompilerParams(collective_id=0, has_side_effects=True, vmem_limit_bytes=2 * 2**20),
            name="step",
        )(*(pltpu.with_memory_space_constraint(a, pltpu.HBM) for a in arrays))
        return tuple(
            pl.pallas_call(
                write_kernel,
                out_shape=[jax.ShapeDtypeStruct(one.shape, one.dtype) for one in new],
                in_specs=[vmem] * 9,
                out_specs=[hbm] * 9,
                scratch_shapes=[dma((9, LAYERS))],
                compiler_params=pltpu.CompilerParams(vmem_limit_bytes=2**18),
                name="write",
            )(*(pltpu.with_memory_space_constraint(a, pltpu.VMEM) for a in new))
        )

    all_of, cut = P(None, None, None), P(None, "dp", None)
    return jax.shard_map(
        step,
        mesh=mesh,
        in_specs=(P(("rep", "dp"), None, None, None),) * 3 + (all_of,) * 3 + (cut,) * 6,
        out_specs=(P("rep", None, None),) * 3 + (P("rep", "dp", None),) * 6,
        check_vma=False,
    )
```

```python
import functools

import jax
import jax.numpy as jnp
from jax import lax
from jax.experimental import pallas as pl
from jax.experimental.pallas import tpu as pltpu
from jax.sharding import PartitionSpec as P

DEVICES = 16
LAYERS = 2
WINDOW = 12
BF16, F32 = jnp.bfloat16, jnp.float32
AXES = ((0, 1, 2), (1, 2, 0), (2, 0, 1))
WIDTH = 1664
VMEM = 67_043_328
SLACK = 300_000
PIECES = 4
UNITS = [(layer, w) for layer in range(LAYERS) for w in range(3)]


def gather_order():
    free, events, order = [0.0, 0.0, 0.0], [], []

    def send(now, layer, w, block):
        for bit in (0, 1, 2):
            if block >> bit or (layer, block, bit) == (1, 3, 2):
                continue
            axis = AXES[w][2 - bit]
            free[axis] = max(free[axis], now) + (0.5 if (layer, block, bit) == (0, 3, 2) else 1.0)
            events.append((free[axis], layer, w, block | 1 << bit))

    for i, (layer, w) in enumerate(UNITS):
        send(0.01 * i, layer, w, 0)
    while events:
        events.sort()
        now, layer, w, block = events.pop(0)
        order.append((layer, w, block))
        send(now + 0.1, layer, w, block)
    return order


def adamw(w, m, v, g):
    m = 0.9 * m + 0.1 * g
    v = 0.95 * v + 0.05 * g * g
    step = m * lax.rsqrt(v + 1e-8) + 0.1 * w
    return (w - 0.02 * step).astype(BF16), m, v


def tiles(rows, columns, body):
    width = WIDTH if columns % WIDTH == 0 else columns

    def step(i, _):
        for c in range(0, columns, width):
            body(pl.ds(pl.multiple_of(i * 16, 16), 16), pl.ds(c, width))

    lax.fori_loop(0, rows // 16, step, None)


def each(n, body):
    lax.fori_loop(0, n, lambda p, _: body(p), None)


def step_kernel(count, *refs):
    g, wt, m_in, v_in = (refs[i : i + 3] for i in (0, 3, 6, 9))
    out, m, v, tail = (refs[i : i + 3] for i in (12, 15, 18, 21))
    wide, tall, squares, all_squares, send_sem, recv_sem, load_sem, in_sem, tile_sem, sum_send, sum_recv, free_sem, cut_send, cut_recv = refs[24:]
    rows = [ref.shape[2] // DEVICES for ref in g]
    columns = [ref.shape[3] for ref in g]

    me = lax.axis_index("dp")
    core = lax.rem(me, 2)
    bits = (me // 8, lax.rem(me // 4, 2), lax.rem(me // 2, 2))
    hop = [(1 - 2 * b) * s for b, s in zip(bits, (8, 4, 2), strict=True)]
    other = 1 - 2 * core

    def away(w, slot):
        return sum(hop[AXES[w][2 - bit]] for bit in range(3) if slot >> bit & 1)

    def block(w, index):
        return pl.ds(pl.multiple_of(index * rows[w], rows[w]), rows[w])

    def part(w, layer, unit):
        return out[w].at[layer, unit * rows[w] : (unit + 1) * rows[w]]

    def copy(w, layer, n, source, target, to):
        return pltpu.make_async_remote_copy(
            src_ref=source,
            dst_ref=target,
            send_sem=send_sem.at[layer * 3 + w, n],
            recv_sem=recv_sem.at[layer * 3 + w, n],
            device_id={"dp": me + to},
            device_id_type=pl.DeviceIdType.MESH,
        )

    def piece(w, ref, p):
        return ref.at[:, pl.ds(pl.multiple_of(p * 256, 256), 256)] if w == 2 else ref.at[pl.ds(pl.multiple_of(p * 16, 16), 16)]

    def cut_copy(kind, n, p, source, target, to, w=None):
        w = n if w is None else w
        return pltpu.make_async_remote_copy(
            src_ref=piece(w, source, p),
            dst_ref=piece(w, target, p),
            send_sem=cut_send.at[kind, n, p],
            recv_sem=cut_recv.at[kind, n, p],
            device_id={"dp": me + to},
            device_id_type=pl.DeviceIdType.MESH,
        )

    def load(w, layer, slot):
        source = g[w].at[0, layer, block(w, me + away(w, slot))]
        return pltpu.make_async_copy(source, part(w, layer, slot + 4), load_sem.at[layer * 3 + w, slot])

    def swap(w, layer, slot):
        source = g[w].at[0, layer, block(w, me + other + away(w, slot))]
        if (layer, slot) == (0, 7):
            return PIECES, lambda p: cut_copy(0, w, p, source, part(w, layer, slot), other)
        return 1, lambda p: copy(w, layer, slot, source, part(w, layer, slot), other)

    def first(w, layer, slot):
        source, target, to = part(w, layer, 4 + slot), part(w, layer, 8 + slot), hop[AXES[w][0]]
        if (layer, slot) == (0, 7):
            return PIECES, lambda p: cut_copy(1, w, p, source, target, to)
        return 1, lambda p: copy(w, layer, 8 + slot - 4, source, target, to)

    def second(w, layer, slot):
        return copy(w, layer, 12 + slot - 2, part(w, layer, slot), part(w, layer, 8 + slot), hop[AXES[w][1]])

    def third(w, layer):
        source, target, to = part(w, layer, 1), part(w, layer, 9), hop[AXES[w][2]]
        if layer == LAYERS - 1:
            return PIECES, lambda p: cut_copy(2, w, p, source, target, to)
        return 1, lambda p: copy(w, layer, 14, source, target, to)

    early = [(w, layer, slot) for layer in range(LAYERS) for slot in (7, 6, 5, 4) for w in range(3)]
    late = [(w, layer, slot) for pair in ((3, 2), (1,), (0,)) for layer in range(LAYERS) for slot in pair for w in range(3)]
    barrier = pltpu.get_barrier_semaphore()
    for to in (other, *hop):
        pl.semaphore_signal(barrier, inc=1, device_id={"dp": me + to}, device_id_type=pl.DeviceIdType.MESH)
    for unit in early[:3]:
        load(*unit).start()
    pl.semaphore_wait(barrier, 4)

    swaps = [swap(*unit) for unit in early + late]
    for p in range(PIECES):
        for w in range(3):
            swaps[w][1](p).start()
    for unit in early[3:6]:
        load(*unit).start()
    for _, c in swaps[3:WINDOW]:
        c(0).start()
    for unit in early[6:]:
        load(*unit).start()

    def done(copies, side):
        n, c = copies
        if n == 1:
            getattr(c(0), side)()
        else:
            each(n, lambda p: getattr(c(p), side)())

    def add_up(sources, r, c):
        acc = sources[0][r, c].astype(F32)
        for s in sources[1:]:
            acc += s[r, c].astype(F32)
        return acc

    def total(sources, target):
        def tile(r, c):
            target[r, c] = add_up(sources, r, c).astype(BF16)

        tiles(*target.shape, tile)

    def join(w, layer, slot, p, swap_copy, first_copy):
        swap_copy.wait_recv()
        mine, theirs = part(w, layer, 4 + slot), part(w, layer, slot)
        if p is not None:
            mine, theirs = piece(w, mine, p), piece(w, theirs, p)
        total([mine, theirs], mine)
        first_copy.start()

    for w in range(3):
        load(w, 0, 7).wait()

    @functools.partial(each, PIECES)
    def _(p):
        for w in range(3):
            join(w, 0, 7, p, swaps[w][1](p), first(w, 0, 7)[1](p))

    for i, (w, layer, slot) in enumerate(early):
        if i >= 3:
            load(w, layer, slot).wait()
            join(w, layer, slot, None, swaps[i][1](0), first(w, layer, slot)[1](0))
        load(w, layer, slot - 4).start()
        if i + WINDOW < len(swaps):
            swaps[i + WINDOW][1](0).start()

    loads = [pltpu.make_async_copy(m_in[w], m[w], in_sem.at[w, 0]) for w in range(3)]
    for c in loads:
        c.start()

    def tile_load(w, layer, i, slot):
        source = v_in[w].at[layer, pl.ds(pl.multiple_of(i * 16, 16), 16)]
        return pltpu.make_async_copy(source, (tall if w == 2 else wide).at[slot], tile_sem.at[int(w == 2), slot])

    for i in range(4):
        tile_load(0, 0, i, i).start()
        tile_load(2, 0, i, i).start()

    squares[...] = jnp.zeros_like(squares)
    freed = set()
    for i, (w, layer, slot) in enumerate(late, len(early)):
        if layer not in freed:
            freed.add(layer)
            for x in range(3):
                for sent_slot in (7, 6, 5):
                    done(first(x, layer, sent_slot), "wait_send")
                for axis in (1, 2):
                    to = {"dp": me + hop[AXES[x][axis]]}
                    pl.semaphore_signal(free_sem.at[layer * 3 + x, axis - 1], inc=1, device_id=to, device_id_type=pl.DeviceIdType.MESH)
        load(w, layer, slot).wait()
        done(swaps[i], "wait_recv")
        done(first(w, layer, slot + 4), "wait_recv")
        sources = [part(w, layer, slot + 4), part(w, layer, slot), part(w, layer, 12 + slot)]
        if slot < 2:
            second(w, layer, slot + 2).wait_recv()
            sources.append(part(w, layer, 10 + slot))
        if slot == 0:

            def tile(r, c, sources=sources, w=w, layer=layer):
                v[w][layer, r, c] = add_up(sources, r, c)

            tiles(rows[w], columns[w], tile)
        elif slot == 1:
            pl.semaphore_wait(free_sem.at[layer * 3 + w, 1], 1)
            n, c = third(w, layer)
            target = part(w, layer, slot)
            if n == 1:
                total(sources, target)
                c(0).start()
            else:

                @functools.partial(each, n)
                def _(p, w=w, c=c, sources=sources, target=target):
                    total([piece(w, ref, p) for ref in sources], piece(w, target, p))
                    c(p).start()

        else:
            total(sources, part(w, layer, slot))
            if slot == 3:
                pl.semaphore_wait(free_sem.at[layer * 3 + w, 0], 1)
            second(w, layer, slot).start()
        if i + WINDOW < len(swaps):
            swaps[i + WINDOW][1](0).start()

    def finish(w, last, grad):
        def tile(r, c):
            rounded = (grad[r, c] + last[r, c].astype(F32)).astype(BF16).astype(F32)
            grad[r, c] = rounded
            squares[:, : c.size] += rounded * rounded

        tiles(*last.shape, tile)

    squares[...] = jnp.zeros_like(squares)
    for w in range(3):
        done(third(w, 0), "wait_recv")
        finish(w, part(w, 0, 9), v[w].at[0])

    for copies in swaps:
        done(copies, "wait_send")
    for layer, w in UNITS:
        done(first(w, layer, 4), "wait_send")
        for slot in (3, 2):
            second(w, layer, slot).wait_send()
    for w in range(3):
        done(third(w, 0), "wait_send")

    @functools.partial(each, PIECES)
    def _(p):
        for w in range(3):
            third(w, 1)[1](p).wait_recv()
            finish(w, piece(w, part(w, 1, 9), p), piece(w, v[w].at[1], p))

    for w in range(3):
        done(third(w, 1), "wait_send")

    everyone = [
        pltpu.make_async_remote_copy(
            src_ref=all_squares.at[0],
            dst_ref=all_squares.at[k],
            send_sem=sum_send.at[k],
            recv_sem=sum_recv.at[k],
            device_id={"dp": lax.rem(me + k, DEVICES)},
            device_id_type=pl.DeviceIdType.MESH,
        )
        for k in range(1, DEVICES)
    ]
    s = squares[:8] + squares[8:]
    all_squares[0] = sum(s[:, c : c + 128] for c in range(0, WIDTH, 128))
    for c in everyone:
        c.start()
    loads += [pltpu.make_async_copy(wt[w].at[:, block(w, me)], out[w].at[:, block(w, me)], in_sem.at[w, 1]) for w in range(3)]
    for c in loads[3:]:
        c.start()
    for c in loads:
        c.wait()
    for c in everyone:
        c.wait_recv()
    s = jnp.sum(jnp.sum(jnp.sum(all_squares[...], axis=0), axis=0, keepdims=True), axis=1, keepdims=True)
    factor = jnp.minimum(1.0, 0.5 * lax.rsqrt(s / count + 1e-30))

    def forward(w, layer, k, bit):
        where = out[w].at[layer, block(w, me + away(w, k))]
        return copy(w, layer, 7 + k if bit == 3 else (k | 1 << bit) - 1, where, where, other if bit == 3 else hop[AXES[w][2 - bit]])

    def forward_cut(bit, p):
        where = out[0].at[0, block(0, me)]
        return cut_copy(5, bit, p, where, where, hop[AXES[0][2 - bit]], 0)

    def arrived_cut(k, p):
        source, target = out[0].at[0, block(0, me)], out[0].at[0, block(0, me + away(0, k))]
        bit = k.bit_length() - 1
        return cut_copy(5, bit, p, source, target, hop[AXES[0][2 - bit]], 0)

    def head(w):
        return rows[w] // 32 * 16

    def rest(w, k, p):
        lo = head(w)
        where = out[w].at[0, block(w, me + away(w, k))]
        if w == 2:
            return where.at[pl.ds(lo, rows[w] - lo), pl.ds(pl.multiple_of(p * 512, 512), 512)]
        return where.at[pl.ds(pl.multiple_of(lo + p * 16, 16), 16)]

    def rest_copy(w, k, p):
        return pltpu.make_async_remote_copy(
            src_ref=rest(w, k, p),
            dst_ref=rest(w, k, p),
            send_sem=cut_send.at[3 if k == 3 else 4, w, p],
            recv_sem=cut_recv.at[3 if k == 3 else 4, w, p],
            device_id={"dp": me + (hop[AXES[w][0]] if k == 3 else other)},
            device_id_type=pl.DeviceIdType.MESH,
        )

    def rest_arrived(w, k, p, to):
        where = rest(w, k, p) if to is None else to
        kind = 3 if to is None else 4
        return pltpu.make_async_remote_copy(
            src_ref=where,
            dst_ref=where,
            send_sem=cut_send.at[kind, w, p],
            recv_sem=cut_recv.at[kind, w, p],
            device_id={"dp": me + other},
            device_id_type=pl.DeviceIdType.MESH,
        )

    def tail_copy(w, layer):
        source = out[w].at[layer, block(w, me + away(w, 3))]
        if layer == 1:
            return pltpu.make_async_copy(source, tail[w].at[: rows[w]], in_sem.at[w, 0])
        return pltpu.make_async_copy(source.at[: head(w)], tail[w].at[rows[w] :], in_sem.at[w, 1])

    def arrived(w, layer, k):
        bit = k.bit_length() - 1
        return copy(w, layer, k - 1, out[w].at[layer, block(w, me)], out[w].at[layer, block(w, me + away(w, k))], hop[AXES[w][2 - bit]])

    sent = []

    def pass_on(w, layer, k):
        for bit in range(4):
            if not k >> bit or bit == 3:
                sent.append(forward(w, layer, k, bit))
                sent[-1].start()

    def advance(w, layer, i):
        slot = i if w < 2 else lax.rem(layer * (rows[w] // 16) + i, 4)
        tile_load(w, layer, i, slot).wait()
        r = pl.ds(pl.multiple_of(i * 16, 16), 16)
        at = pl.ds(pl.multiple_of(me * rows[w] + i * 16, 16), 16)
        for column in range(0, columns[w], 256):
            c = pl.ds(column, 256)
            old = (tall if w == 2 else wide)[slot, :, c]
            new, m[w][layer, r, c], v[w][layer, r, c] = adamw(
                out[w][layer, at, c].astype(F32), m[w][layer, r, c], old, v[w][layer, r, c] * factor
            )
            out[w][layer, at, c] = new
        if w == 0:
            tile_load(1, layer, i, slot).start()
        elif w == 1 and layer + 1 < LAYERS:
            tile_load(0, layer + 1, i, slot).start()
        elif w == 2:
            ahead = i + 4

            @pl.when(ahead < rows[w] // 16)
            def _():
                tile_load(w, layer, ahead, slot).start()

            if layer + 1 < LAYERS:

                @pl.when(ahead >= rows[w] // 16)
                def _():
                    tile_load(w, layer + 1, ahead - rows[w] // 16, slot).start()

    for layer, w in UNITS:
        if (layer, w) == (0, 0):

            @functools.partial(each, PIECES)
            def _(p):
                advance(0, 0, p)
                for bit in range(3):
                    forward_cut(bit, p).start()

            sent.append(forward(w, layer, 0, 3))
            sent[-1].start()
        else:
            lax.fori_loop(0, rows[w] // 16, lambda i, _, w=w, layer=layer: advance(w, layer, i), None)
            pass_on(w, layer, 0)
    order = gather_order()
    last = [(0, w, 7) for w in range(3)]
    assert sorted(order[-3:]) == last
    for layer, w, k in order[:-3]:
        if (layer, w) == (0, 0) and k & k - 1 == 0:
            each(PIECES, lambda p, k=k: arrived_cut(k, p).wait_recv())
        else:
            arrived(w, layer, k).wait_recv()
        if k == 3:
            if layer == 0:
                each(2, lambda p, w=w: rest_copy(w, 3, p).start())
            tail_copy(w, layer).start()
            sent.append(forward(w, layer, k, 3))
            sent[-1].start()
        else:
            pass_on(w, layer, k)

    for layer, w in UNITS:
        for k in range(7):
            where = out[w].at[layer, block(w, me + other + away(w, k))]
            copy(w, layer, 7 + k, where, where, other).wait_recv()
    for c in sent:
        c.wait_send()
    for c in everyone:
        c.wait_send()
    for bit in range(3):
        each(PIECES, lambda p, bit=bit: forward_cut(bit, p).wait_send())
    for w in range(3):
        for layer in range(LAYERS):
            tail_copy(w, layer).wait()

    @functools.partial(each, 2)
    def _(p):
        for w in range(3):
            rest_arrived(w, 7, p, None).wait_recv()
            rest_copy(w, 7, p).start()

    def theirs(w, p):
        lo = head(w)
        where = out[w].at[0, block(w, me + other + away(w, 7))]
        if w == 2:
            return where.at[pl.ds(lo, rows[w] - lo), pl.ds(pl.multiple_of(p * 512, 512), 512)]
        return where.at[pl.ds(pl.multiple_of(lo + p * 16, 16), 16)]

    @functools.partial(each, 2)
    def _(p):
        for w in range(3):
            rest_arrived(w, 7, p, theirs(w, p)).wait_recv()
            rest_copy(w, 3, p).wait_send()
            rest_copy(w, 7, p).wait_send()


def write_kernel(n, *refs):
    sem = refs[2 * n]
    copies = [pltpu.make_async_copy(refs[i].at[layer], refs[n + i].at[layer], sem.at[i, layer]) for i in range(n) for layer in range(LAYERS)]
    for c in copies:
        c.start()
    for c in copies:
        c.wait()


def write(new, held):
    n = len(new)
    size = sum(one.size * one.dtype.itemsize for one in new)
    return pl.pallas_call(
        functools.partial(write_kernel, n),
        out_shape=[jax.ShapeDtypeStruct(one.shape, one.dtype) for one in new],
        in_specs=[pl.BlockSpec(memory_space=pltpu.VMEM)] * n,
        out_specs=[pl.BlockSpec(memory_space=pltpu.HBM)] * n,
        scratch_shapes=[pltpu.SemaphoreType.DMA((n, LAYERS))],
        compiler_params=pltpu.CompilerParams(vmem_limit_bytes=VMEM - held - SLACK),
        cost_estimate=pl.CostEstimate(flops=size * 4, bytes_accessed=size, transcendentals=0),
        name="write",
    )(*(pltpu.with_memory_space_constraint(a, pltpu.VMEM) for a in new))


def tail_kernel(blocks, *refs):
    out, held, sem, in_sem = refs[9:12], refs[12:15], refs[15], refs[16]
    loads = [pltpu.make_async_copy(refs[i], held[i], in_sem.at[i]) for i in range(3)]
    for c in loads:
        c.start()
    tails = (*held, *refs[3:6])
    me = lax.axis_index("dp")
    other = 1 - 2 * lax.rem(me, 2)
    far = 14 - 2 * (me // 2)
    copies = []
    for i in (3, 4, 5, 0, 1, 2):
        source, n = tails[i], blocks[i % 3]
        if i < 3:
            loads[i].wait()
        start = (far + lax.rem(me + (other if i >= 3 else 0), 2)) * n
        for layer, (lo, size) in ((1, (0, n)), (0, (n, source.shape[0] - n))):
            target = out[i % 3].at[layer, pl.ds(pl.multiple_of(start, 16), size)]
            copies.append(pltpu.make_async_copy(source.at[lo : lo + size], target, sem.at[i, layer]))
            copies[-1].start()
    for c in copies:
        c.wait()


def solution(mesh):
    def step(*arrays):
        weights, moments = arrays[3:6], arrays[6:12]
        blocks = [one.shape for one in moments[:3]]
        new = [pltpu.VMEM(w.shape, BF16) for w in weights] + [pltpu.VMEM(one.shape, F32) for one in moments]
        new += [pltpu.HBM((b[1] + b[1] // 32 * 16, b[2]), BF16) for b in blocks]
        held = sum(one.size * one.dtype.itemsize for one in (*weights, *moments))
        hbm, vmem = pl.BlockSpec(memory_space=pltpu.HBM), pl.BlockSpec(memory_space=pltpu.VMEM)
        dma = pltpu.SemaphoreType.DMA
        count = float(sum(w.size for w in weights))
        new = pl.pallas_call(
            functools.partial(step_kernel, count),
            out_shape=new,
            in_specs=[hbm] * 12,
            out_specs=[vmem] * 9 + [hbm] * 3,
            scratch_shapes=[
                pltpu.VMEM((4, 16, blocks[0][2]), F32),
                pltpu.VMEM((4, 16, blocks[2][2]), F32),
                pltpu.VMEM((16, WIDTH), F32),
                pltpu.VMEM((DEVICES, 8, 128), F32),
                dma((6, 15)),
                dma((6, 15)),
                dma((6, 8)),
                dma((3, 2)),
                dma((2, 4)),
                dma((DEVICES,)),
                dma((DEVICES,)),
                pltpu.SemaphoreType.REGULAR((6, 2)),
                dma((6, 3, PIECES)),
                dma((6, 3, PIECES)),
            ],
            compiler_params=pltpu.CompilerParams(collective_id=0, has_side_effects=True, vmem_limit_bytes=VMEM - held - SLACK),
            name="step",
        )(*(pltpu.with_memory_space_constraint(a, pltpu.HBM) for a in arrays))
        new, tails = new[:9], new[9:]
        mine = [lax.ppermute(t, "dp", [(i, i ^ (8, 4, 2)[AXES[w][0]]) for i in range(DEVICES)]) for w, t in enumerate(tails)]
        gate, up, down, *moments = write(new, held)
        *mine, gate = lax.optimization_barrier((*mine, gate))
        theirs = [lax.ppermute(t, "dp", [(i, i ^ 1) for i in range(DEVICES)]) for t in mine]
        whole = pl.pallas_call(
            functools.partial(tail_kernel, [b[1] for b in blocks]),
            out_shape=[jax.ShapeDtypeStruct(one.shape, one.dtype) for one in weights],
            in_specs=[hbm] * 3 + [vmem] * 3 + [hbm] * 3,
            out_specs=[hbm] * 3,
            input_output_aliases={6: 0, 7: 1, 8: 2},
            scratch_shapes=[*(pltpu.VMEM(t.shape, BF16) for t in tails), dma((6, LAYERS)), dma((3,))],
            compiler_params=pltpu.CompilerParams(vmem_limit_bytes=5 * 2**20),
            name="tail",
        )(
            *(pltpu.with_memory_space_constraint(a, pltpu.HBM) for a in mine),
            *(pltpu.with_memory_space_constraint(a, pltpu.VMEM) for a in theirs),
            gate,
            up,
            down,
        )
        return (*whole, *moments)

    all_of, cut = P(None, None, None), P(None, "dp", None)
    return jax.shard_map(
        step,
        mesh=mesh,
        in_specs=(P(("rep", "dp"), None, None, None),) * 3 + (all_of,) * 3 + (cut,) * 6,
        out_specs=(P("rep", None, None),) * 3 + (P("rep", "dp", None),) * 6,
        check_vma=False,
    )
```

```python
import functools

import jax
import jax.numpy as jnp
from jax import lax
from jax.experimental import pallas as pl
from jax.experimental.pallas import tpu as pltpu
from jax.sharding import PartitionSpec as P

DEVICES = 16
LAYERS = 2
WINDOW = 12
BF16, F32 = jnp.bfloat16, jnp.float32
AXES = ((0, 1, 2), (1, 2, 0), (2, 0, 1))
WIDTH = 1664
VMEM = 67_043_328
SLACK = 300_000
PIECES = 4
UNITS = [(layer, w) for layer in range(LAYERS) for w in range(3)]


def head_rows(rows):
    return rows // 16 * 3 // 4 * 16


def gather_order():
    free, events, order = [0.0, 0.0, 0.0], [], []

    def send(now, layer, w, block):
        for bit in (0, 1, 2):
            if block >> bit or (layer, block, bit) == (1, 3, 2):
                continue
            axis = AXES[w][2 - bit]
            free[axis] = max(free[axis], now) + (0.25 if (layer, block, bit) == (0, 3, 2) else 1.0)
            events.append((free[axis], layer, w, block | 1 << bit))

    for i, (layer, w) in enumerate(UNITS):
        send(0.01 * i, layer, w, 0)
    while events:
        events.sort()
        now, layer, w, block = events.pop(0)
        order.append((layer, w, block))
        send(now + 0.1, layer, w, block)
    return order


def adamw(w, m, v, g):
    m = 0.9 * m + 0.1 * g
    v = 0.95 * v + 0.05 * g * g
    step = m * lax.rsqrt(v + 1e-8) + 0.1 * w
    return (w - 0.02 * step).astype(BF16), m, v


def tiles(rows, columns, body):
    width = WIDTH if columns % WIDTH == 0 else columns

    def step(i, _):
        for c in range(0, columns, width):
            body(pl.ds(pl.multiple_of(i * 16, 16), 16), pl.ds(c, width))

    lax.fori_loop(0, rows // 16, step, None)


def each(n, body):
    lax.fori_loop(0, n, lambda p, _: body(p), None)


def step_kernel(count, *refs):
    g, wt, m_in, v_in = (refs[i : i + 3] for i in (0, 3, 6, 9))
    out, m, v, tail = (refs[i : i + 3] for i in (12, 15, 18, 21))
    wide, tall, squares, all_squares, send_sem, recv_sem, load_sem, in_sem, tile_sem, sum_send, sum_recv, free_sem, cut_send, cut_recv = refs[24:]
    rows = [ref.shape[2] // DEVICES for ref in g]
    columns = [ref.shape[3] for ref in g]

    me = lax.axis_index("dp")
    core = lax.rem(me, 2)
    bits = (me // 8, lax.rem(me // 4, 2), lax.rem(me // 2, 2))
    hop = [(1 - 2 * b) * s for b, s in zip(bits, (8, 4, 2), strict=True)]
    other = 1 - 2 * core

    def away(w, slot):
        return sum(hop[AXES[w][2 - bit]] for bit in range(3) if slot >> bit & 1)

    def block(w, index):
        return pl.ds(pl.multiple_of(index * rows[w], rows[w]), rows[w])

    def part(w, layer, unit):
        return out[w].at[layer, unit * rows[w] : (unit + 1) * rows[w]]

    def copy(w, layer, n, source, target, to):
        return pltpu.make_async_remote_copy(
            src_ref=source,
            dst_ref=target,
            send_sem=send_sem.at[layer * 3 + w, n],
            recv_sem=recv_sem.at[layer * 3 + w, n],
            device_id={"dp": me + to},
            device_id_type=pl.DeviceIdType.MESH,
        )

    def piece(w, ref, p):
        return ref.at[:, pl.ds(pl.multiple_of(p * 256, 256), 256)] if w == 2 else ref.at[pl.ds(pl.multiple_of(p * 16, 16), 16)]

    def cut_copy(kind, n, p, source, target, to, w=None):
        w = n if w is None else w
        return pltpu.make_async_remote_copy(
            src_ref=piece(w, source, p),
            dst_ref=piece(w, target, p),
            send_sem=cut_send.at[kind, n, p],
            recv_sem=cut_recv.at[kind, n, p],
            device_id={"dp": me + to},
            device_id_type=pl.DeviceIdType.MESH,
        )

    def load(w, layer, slot):
        source = g[w].at[0, layer, block(w, me + away(w, slot))]
        return pltpu.make_async_copy(source, part(w, layer, slot + 4), load_sem.at[layer * 3 + w, slot])

    def swap(w, layer, slot):
        source = g[w].at[0, layer, block(w, me + other + away(w, slot))]
        if (layer, slot) == (0, 7):
            return PIECES, lambda p: cut_copy(0, w, p, source, part(w, layer, slot), other)
        return 1, lambda p: copy(w, layer, slot, source, part(w, layer, slot), other)

    def first(w, layer, slot):
        source, target, to = part(w, layer, 4 + slot), part(w, layer, 8 + slot), hop[AXES[w][0]]
        if (layer, slot) == (0, 7):
            return PIECES, lambda p: cut_copy(1, w, p, source, target, to)
        return 1, lambda p: copy(w, layer, 8 + slot - 4, source, target, to)

    def second(w, layer, slot):
        return copy(w, layer, 12 + slot - 2, part(w, layer, slot), part(w, layer, 8 + slot), hop[AXES[w][1]])

    def third(w, layer):
        source, target, to = part(w, layer, 1), part(w, layer, 9), hop[AXES[w][2]]
        if layer == LAYERS - 1:
            return PIECES, lambda p: cut_copy(2, w, p, source, target, to)
        return 1, lambda p: copy(w, layer, 14, source, target, to)

    early = [(w, layer, slot) for layer in range(LAYERS) for slot in (7, 6, 5, 4) for w in range(3)]
    late = [(w, layer, slot) for pair in ((3, 2), (1,), (0,)) for layer in range(LAYERS) for slot in pair for w in range(3)]
    barrier = pltpu.get_barrier_semaphore()
    for to in (other, *hop):
        pl.semaphore_signal(barrier, inc=1, device_id={"dp": me + to}, device_id_type=pl.DeviceIdType.MESH)
    for unit in early[:3]:
        load(*unit).start()
    pl.semaphore_wait(barrier, 4)

    swaps = [swap(*unit) for unit in early + late]
    for p in range(PIECES):
        for w in range(3):
            swaps[w][1](p).start()
    for unit in early[3:6]:
        load(*unit).start()
    for _, c in swaps[3:WINDOW]:
        c(0).start()
    for unit in early[6:]:
        load(*unit).start()

    def done(copies, side):
        n, c = copies
        if n == 1:
            getattr(c(0), side)()
        else:
            each(n, lambda p: getattr(c(p), side)())

    def add_up(sources, r, c):
        acc = sources[0][r, c].astype(F32)
        for s in sources[1:]:
            acc += s[r, c].astype(F32)
        return acc

    def total(sources, target):
        def tile(r, c):
            target[r, c] = add_up(sources, r, c).astype(BF16)

        tiles(*target.shape, tile)

    def join(w, layer, slot, p, swap_copy, first_copy):
        swap_copy.wait_recv()
        mine, theirs = part(w, layer, 4 + slot), part(w, layer, slot)
        if p is not None:
            mine, theirs = piece(w, mine, p), piece(w, theirs, p)
        total([mine, theirs], mine)
        first_copy.start()

    for w in range(3):
        load(w, 0, 7).wait()

    @functools.partial(each, PIECES)
    def _(p):
        for w in range(3):
            join(w, 0, 7, p, swaps[w][1](p), first(w, 0, 7)[1](p))

    for i, (w, layer, slot) in enumerate(early):
        if i >= 3:
            load(w, layer, slot).wait()
            join(w, layer, slot, None, swaps[i][1](0), first(w, layer, slot)[1](0))
        load(w, layer, slot - 4).start()
        if i + WINDOW < len(swaps):
            swaps[i + WINDOW][1](0).start()

    loads = [pltpu.make_async_copy(m_in[w], m[w], in_sem.at[w, 0]) for w in range(3)]
    for c in loads:
        c.start()

    def tile_load(w, layer, i, slot):
        source = v_in[w].at[layer, pl.ds(pl.multiple_of(i * 16, 16), 16)]
        return pltpu.make_async_copy(source, (tall if w == 2 else wide).at[slot], tile_sem.at[int(w == 2), slot])

    for i in range(4):
        tile_load(0, 0, i, i).start()
        tile_load(2, 0, i, i).start()

    squares[...] = jnp.zeros_like(squares)
    freed = set()
    for i, (w, layer, slot) in enumerate(late, len(early)):
        if layer not in freed:
            freed.add(layer)
            for x in range(3):
                for sent_slot in (7, 6, 5):
                    done(first(x, layer, sent_slot), "wait_send")
                for axis in (1, 2):
                    to = {"dp": me + hop[AXES[x][axis]]}
                    pl.semaphore_signal(free_sem.at[layer * 3 + x, axis - 1], inc=1, device_id=to, device_id_type=pl.DeviceIdType.MESH)
        load(w, layer, slot).wait()
        done(swaps[i], "wait_recv")
        done(first(w, layer, slot + 4), "wait_recv")
        sources = [part(w, layer, slot + 4), part(w, layer, slot), part(w, layer, 12 + slot)]
        if slot < 2:
            second(w, layer, slot + 2).wait_recv()
            sources.append(part(w, layer, 10 + slot))
        if slot == 0:

            def tile(r, c, sources=sources, w=w, layer=layer):
                v[w][layer, r, c] = add_up(sources, r, c)

            tiles(rows[w], columns[w], tile)
        elif slot == 1:
            pl.semaphore_wait(free_sem.at[layer * 3 + w, 1], 1)
            n, c = third(w, layer)
            target = part(w, layer, slot)
            if n == 1:
                total(sources, target)
                c(0).start()
            else:

                @functools.partial(each, n)
                def _(p, w=w, c=c, sources=sources, target=target):
                    total([piece(w, ref, p) for ref in sources], piece(w, target, p))
                    c(p).start()

        else:
            total(sources, part(w, layer, slot))
            if slot == 3:
                pl.semaphore_wait(free_sem.at[layer * 3 + w, 0], 1)
            second(w, layer, slot).start()
        if i + WINDOW < len(swaps):
            swaps[i + WINDOW][1](0).start()

    def finish(w, last, grad):
        def tile(r, c):
            rounded = (grad[r, c] + last[r, c].astype(F32)).astype(BF16).astype(F32)
            grad[r, c] = rounded
            squares[:, : c.size] += rounded * rounded

        tiles(*last.shape, tile)

    squares[...] = jnp.zeros_like(squares)
    for w in range(3):
        done(third(w, 0), "wait_recv")
        finish(w, part(w, 0, 9), v[w].at[0])

    for copies in swaps:
        done(copies, "wait_send")
    for layer, w in UNITS:
        done(first(w, layer, 4), "wait_send")
        for slot in (3, 2):
            second(w, layer, slot).wait_send()
    for w in range(3):
        done(third(w, 0), "wait_send")

    @functools.partial(each, PIECES)
    def _(p):
        for w in range(3):
            third(w, 1)[1](p).wait_recv()
            finish(w, piece(w, part(w, 1, 9), p), piece(w, v[w].at[1], p))

    for w in range(3):
        done(third(w, 1), "wait_send")

    everyone = [
        pltpu.make_async_remote_copy(
            src_ref=all_squares.at[0],
            dst_ref=all_squares.at[k],
            send_sem=sum_send.at[k],
            recv_sem=sum_recv.at[k],
            device_id={"dp": lax.rem(me + k, DEVICES)},
            device_id_type=pl.DeviceIdType.MESH,
        )
        for k in range(1, DEVICES)
    ]
    s = squares[:8] + squares[8:]
    all_squares[0] = sum(s[:, c : c + 128] for c in range(0, WIDTH, 128))
    for c in everyone:
        c.start()
    loads += [pltpu.make_async_copy(wt[w].at[:, block(w, me)], out[w].at[:, block(w, me)], in_sem.at[w, 1]) for w in range(3)]
    for c in loads[3:]:
        c.start()
    for c in loads:
        c.wait()
    for c in everyone:
        c.wait_recv()
    s = jnp.sum(jnp.sum(jnp.sum(all_squares[...], axis=0), axis=0, keepdims=True), axis=1, keepdims=True)
    factor = jnp.minimum(1.0, 0.5 * lax.rsqrt(s / count + 1e-30))

    def forward(w, layer, k, bit):
        where = out[w].at[layer, block(w, me + away(w, k))]
        return copy(w, layer, 7 + k if bit == 3 else (k | 1 << bit) - 1, where, where, other if bit == 3 else hop[AXES[w][2 - bit]])

    def forward_cut(bit, p):
        where = out[0].at[0, block(0, me)]
        return cut_copy(5, bit, p, where, where, hop[AXES[0][2 - bit]], 0)

    def arrived_cut(k, p):
        source, target = out[0].at[0, block(0, me)], out[0].at[0, block(0, me + away(0, k))]
        bit = k.bit_length() - 1
        return cut_copy(5, bit, p, source, target, hop[AXES[0][2 - bit]], 0)

    def head(w):
        return head_rows(rows[w])

    def rest(w, k, p):
        lo = head(w)
        where = out[w].at[0, block(w, me + away(w, k))]
        return where.at[pl.ds(lo, rows[w] - lo), pl.ds(pl.multiple_of(p * (columns[w] // 2), 128), columns[w] // 2)]

    def rest_copy(w, k, p):
        return pltpu.make_async_remote_copy(
            src_ref=rest(w, k, p),
            dst_ref=rest(w, k, p),
            send_sem=cut_send.at[3 if k == 3 else 4, w, p],
            recv_sem=cut_recv.at[3 if k == 3 else 4, w, p],
            device_id={"dp": me + (hop[AXES[w][0]] if k == 3 else other)},
            device_id_type=pl.DeviceIdType.MESH,
        )

    def rest_arrived(w, k, p, to):
        where = rest(w, k, p) if to is None else to
        kind = 3 if to is None else 4
        return pltpu.make_async_remote_copy(
            src_ref=where,
            dst_ref=where,
            send_sem=cut_send.at[kind, w, p],
            recv_sem=cut_recv.at[kind, w, p],
            device_id={"dp": me + other},
            device_id_type=pl.DeviceIdType.MESH,
        )

    def tail_copy(w, layer):
        source = out[w].at[layer, block(w, me + away(w, 3))]
        if layer == 1:
            return pltpu.make_async_copy(source, tail[w].at[: rows[w]], in_sem.at[w, 0])
        return pltpu.make_async_copy(source.at[: head(w)], tail[w].at[rows[w] :], in_sem.at[w, 1])

    def arrived(w, layer, k):
        bit = k.bit_length() - 1
        return copy(w, layer, k - 1, out[w].at[layer, block(w, me)], out[w].at[layer, block(w, me + away(w, k))], hop[AXES[w][2 - bit]])

    sent = []

    def pass_on(w, layer, k):
        for bit in range(4):
            if not k >> bit or bit == 3:
                sent.append(forward(w, layer, k, bit))
                sent[-1].start()

    def advance(w, layer, i):
        slot = i if w < 2 else lax.rem(layer * (rows[w] // 16) + i, 4)
        tile_load(w, layer, i, slot).wait()
        r = pl.ds(pl.multiple_of(i * 16, 16), 16)
        at = pl.ds(pl.multiple_of(me * rows[w] + i * 16, 16), 16)
        for column in range(0, columns[w], 256):
            c = pl.ds(column, 256)
            old = (tall if w == 2 else wide)[slot, :, c]
            new, m[w][layer, r, c], v[w][layer, r, c] = adamw(
                out[w][layer, at, c].astype(F32), m[w][layer, r, c], old, v[w][layer, r, c] * factor
            )
            out[w][layer, at, c] = new
        if w == 0:
            tile_load(1, layer, i, slot).start()
        elif w == 1 and layer + 1 < LAYERS:
            tile_load(0, layer + 1, i, slot).start()
        elif w == 2:
            ahead = i + 4

            @pl.when(ahead < rows[w] // 16)
            def _():
                tile_load(w, layer, ahead, slot).start()

            if layer + 1 < LAYERS:

                @pl.when(ahead >= rows[w] // 16)
                def _():
                    tile_load(w, layer + 1, ahead - rows[w] // 16, slot).start()

    for layer, w in UNITS:
        if (layer, w) == (0, 0):

            @functools.partial(each, PIECES)
            def _(p):
                advance(0, 0, p)
                for bit in range(3):
                    forward_cut(bit, p).start()

            sent.append(forward(w, layer, 0, 3))
            sent[-1].start()
        else:
            lax.fori_loop(0, rows[w] // 16, lambda i, _, w=w, layer=layer: advance(w, layer, i), None)
            pass_on(w, layer, 0)
    order = gather_order()
    last = [(0, w, 7) for w in range(3)]
    assert sorted(order[-3:]) == last
    for layer, w, k in order[:-3]:
        if (layer, w) == (0, 0) and k & k - 1 == 0:
            each(PIECES, lambda p, k=k: arrived_cut(k, p).wait_recv())
        else:
            arrived(w, layer, k).wait_recv()
        if k == 3:
            if layer == 0:
                each(2, lambda p, w=w: rest_copy(w, 3, p).start())
            tail_copy(w, layer).start()
            sent.append(forward(w, layer, k, 3))
            sent[-1].start()
        else:
            pass_on(w, layer, k)

    for layer, w in UNITS:
        for k in range(7):
            where = out[w].at[layer, block(w, me + other + away(w, k))]
            copy(w, layer, 7 + k, where, where, other).wait_recv()
    for c in sent:
        c.wait_send()
    for c in everyone:
        c.wait_send()
    for bit in range(3):
        each(PIECES, lambda p, bit=bit: forward_cut(bit, p).wait_send())
    for w in range(3):
        for layer in range(LAYERS):
            tail_copy(w, layer).wait()

    @functools.partial(each, 2)
    def _(p):
        for w in range(3):
            rest_arrived(w, 7, p, None).wait_recv()
            rest_copy(w, 7, p).start()

    def theirs(w, p):
        lo = head(w)
        where = out[w].at[0, block(w, me + other + away(w, 7))]
        return where.at[pl.ds(lo, rows[w] - lo), pl.ds(pl.multiple_of(p * (columns[w] // 2), 128), columns[w] // 2)]

    @functools.partial(each, 2)
    def _(p):
        for w in range(3):
            rest_arrived(w, 7, p, theirs(w, p)).wait_recv()
            rest_copy(w, 3, p).wait_send()
            rest_copy(w, 7, p).wait_send()


def write_kernel(n, *refs):
    sem = refs[2 * n]
    copies = [pltpu.make_async_copy(refs[i].at[layer], refs[n + i].at[layer], sem.at[i, layer]) for i in range(n) for layer in range(LAYERS)]
    for c in copies:
        c.start()
    for c in copies:
        c.wait()


def write(new, held):
    n = len(new)
    size = sum(one.size * one.dtype.itemsize for one in new)
    return pl.pallas_call(
        functools.partial(write_kernel, n),
        out_shape=[jax.ShapeDtypeStruct(one.shape, one.dtype) for one in new],
        in_specs=[pl.BlockSpec(memory_space=pltpu.VMEM)] * n,
        out_specs=[pl.BlockSpec(memory_space=pltpu.HBM)] * n,
        scratch_shapes=[pltpu.SemaphoreType.DMA((n, LAYERS))],
        compiler_params=pltpu.CompilerParams(vmem_limit_bytes=VMEM - held - SLACK),
        cost_estimate=pl.CostEstimate(flops=size * 4, bytes_accessed=size, transcendentals=0),
        name="write",
    )(*(pltpu.with_memory_space_constraint(a, pltpu.VMEM) for a in new))


def tail_kernel(blocks, staged, *refs):
    tails, out, sem = refs[:3], refs[6:9], refs[9]
    me = lax.axis_index("dp")
    far = 14 - 2 * (me // 2)
    at = far + (lax.rem(me, 2) if staged else 1 - lax.rem(me, 2))
    loads = []
    if staged:
        loads = [pltpu.make_async_copy(refs[i], refs[11 + i], refs[10].at[i]) for i in range(3)]
        tails = refs[11:14]
        for c in loads:
            c.start()
    copies = []
    for i, source in enumerate(tails):
        n = blocks[i]
        if loads:
            loads[i].wait()
        for layer, (lo, size) in ((1, (0, n)), (0, (n, source.shape[0] - n))):
            target = out[i].at[layer, pl.ds(pl.multiple_of(at * n, 16), size)]
            copies.append(pltpu.make_async_copy(source.at[lo : lo + size], target, sem.at[i, layer]))
            copies[-1].start()
    for c in copies:
        c.wait()


def put(tails, whole, staged):
    hbm, vmem = pl.BlockSpec(memory_space=pltpu.HBM), pl.BlockSpec(memory_space=pltpu.VMEM)
    space, dma = (pltpu.HBM if staged else pltpu.VMEM), pltpu.SemaphoreType.DMA
    size = sum(t.size for t in tails)
    return pl.pallas_call(
        functools.partial(tail_kernel, [one.shape[1] // DEVICES for one in whole], staged),
        out_shape=[jax.ShapeDtypeStruct(one.shape, one.dtype) for one in whole],
        in_specs=[hbm if staged else vmem] * 3 + [hbm] * 3,
        out_specs=[hbm] * 3,
        input_output_aliases={3: 0, 4: 1, 5: 2},
        scratch_shapes=[dma((3, LAYERS)), dma((3,))] + [pltpu.VMEM(t.shape, BF16) for t in tails if staged],
        compiler_params=pltpu.CompilerParams(vmem_limit_bytes=6 * 2**20),
        cost_estimate=pl.CostEstimate(flops=size * 8, bytes_accessed=size * 4, transcendentals=0),
        name="put",
    )(*(pltpu.with_memory_space_constraint(t, space) for t in tails), *whole)


def solution(mesh):
    def step(*arrays):
        weights, moments = arrays[3:6], arrays[6:12]
        blocks = [one.shape for one in moments[:3]]
        new = [pltpu.VMEM(w.shape, BF16) for w in weights] + [pltpu.VMEM(one.shape, F32) for one in moments]
        new += [pltpu.HBM((b[1] + head_rows(b[1]), b[2]), BF16) for b in blocks]
        held = sum(one.size * one.dtype.itemsize for one in (*weights, *moments))
        hbm, vmem = pl.BlockSpec(memory_space=pltpu.HBM), pl.BlockSpec(memory_space=pltpu.VMEM)
        dma = pltpu.SemaphoreType.DMA
        count = float(sum(w.size for w in weights))
        new = pl.pallas_call(
            functools.partial(step_kernel, count),
            out_shape=new,
            in_specs=[hbm] * 12,
            out_specs=[vmem] * 9 + [hbm] * 3,
            scratch_shapes=[
                pltpu.VMEM((4, 16, blocks[0][2]), F32),
                pltpu.VMEM((4, 16, blocks[2][2]), F32),
                pltpu.VMEM((16, WIDTH), F32),
                pltpu.VMEM((DEVICES, 8, 128), F32),
                dma((6, 15)),
                dma((6, 15)),
                dma((6, 8)),
                dma((3, 2)),
                dma((2, 4)),
                dma((DEVICES,)),
                dma((DEVICES,)),
                pltpu.SemaphoreType.REGULAR((6, 2)),
                dma((6, 3, PIECES)),
                dma((6, 3, PIECES)),
            ],
            compiler_params=pltpu.CompilerParams(collective_id=0, has_side_effects=True, vmem_limit_bytes=VMEM - held - SLACK),
            name="step",
        )(*(pltpu.with_memory_space_constraint(a, pltpu.HBM) for a in arrays))
        new, tails = new[:9], new[9:]
        mine = [lax.ppermute(t, "dp", [(i, i ^ (8, 4, 2)[AXES[w][0]]) for i in range(DEVICES)]) for w, t in enumerate(tails)]
        gate, up, down, *moments = write(new, held)
        *mine, gate = lax.optimization_barrier((*mine, gate))
        theirs = [lax.ppermute(t, "dp", [(i, i ^ 1) for i in range(DEVICES)]) for t in mine]
        whole = put(theirs, put(mine, [gate, up, down], True), False)
        return (*whole, *moments)

    all_of, cut = P(None, None, None), P(None, "dp", None)
    return jax.shard_map(
        step,
        mesh=mesh,
        in_specs=(P(("rep", "dp"), None, None, None),) * 3 + (all_of,) * 3 + (cut,) * 6,
        out_specs=(P("rep", None, None),) * 3 + (P("rep", "dp", None),) * 6,
        check_vma=False,
    )
```

```python
import functools

import jax
import jax.numpy as jnp
from jax import lax
from jax.experimental import pallas as pl
from jax.experimental.pallas import tpu as pltpu
from jax.sharding import PartitionSpec as P

DEVICES = 16
LAYERS = 2
WINDOW = 12
BF16, F32 = jnp.bfloat16, jnp.float32
AXES = ((0, 1, 2), (1, 2, 0), (2, 0, 1))
WIDTH = 1664
VMEM = 67_043_328
SLACK = 300_000
PIECES = 4
UNITS = [(layer, w) for layer in range(LAYERS) for w in range(3)]


def head_rows(rows):
    return rows // 16 * 3 // 4 * 16


def gather_order():
    free, events, order = [0.0, 0.0, 0.0], [], []

    def send(now, layer, w, block):
        for bit in (0, 1, 2):
            if block >> bit or (layer, block, bit) == (1, 3, 2):
                continue
            axis = AXES[w][2 - bit]
            free[axis] = max(free[axis], now) + (0.25 if (layer, block, bit) == (0, 3, 2) else 1.0)
            events.append((free[axis], layer, w, block | 1 << bit))

    for i, (layer, w) in enumerate(UNITS):
        send(0.01 * i, layer, w, 0)
    while events:
        events.sort()
        now, layer, w, block = events.pop(0)
        order.append((layer, w, block))
        send(now + 0.1, layer, w, block)
    return order


def adamw(w, m, v, g):
    m = 0.9 * m + 0.1 * g
    v = 0.95 * v + 0.05 * g * g
    step = m * lax.rsqrt(v + 1e-8) + 0.1 * w
    return (w - 0.02 * step).astype(BF16), m, v


def tiles(rows, columns, body):
    width = WIDTH if columns % WIDTH == 0 else columns

    def step(i, _):
        for c in range(0, columns, width):
            body(pl.ds(pl.multiple_of(i * 16, 16), 16), pl.ds(c, width))

    lax.fori_loop(0, rows // 16, step, None)


def each(n, body):
    lax.fori_loop(0, n, lambda p, _: body(p), None)


def step_kernel(count, *refs):
    g, wt, m_in, v_in = (refs[i : i + 3] for i in (0, 3, 6, 9))
    out, m, v, tail = (refs[i : i + 3] for i in (12, 15, 18, 21))
    wide, tall, squares, all_squares, send_sem, recv_sem, load_sem, in_sem, tile_sem, sum_send, sum_recv, free_sem, cut_send, cut_recv = refs[24:]
    rows = [ref.shape[2] // DEVICES for ref in g]
    columns = [ref.shape[3] for ref in g]

    me = lax.axis_index("dp")
    core = lax.rem(me, 2)
    bits = (me // 8, lax.rem(me // 4, 2), lax.rem(me // 2, 2))
    hop = [(1 - 2 * b) * s for b, s in zip(bits, (8, 4, 2), strict=True)]
    other = 1 - 2 * core

    def away(w, slot):
        return sum(hop[AXES[w][2 - bit]] for bit in range(3) if slot >> bit & 1)

    def block(w, index):
        return pl.ds(pl.multiple_of(index * rows[w], rows[w]), rows[w])

    def part(w, layer, unit):
        return out[w].at[layer, unit * rows[w] : (unit + 1) * rows[w]]

    def copy(w, layer, n, source, target, to):
        return pltpu.make_async_remote_copy(
            src_ref=source,
            dst_ref=target,
            send_sem=send_sem.at[layer * 3 + w, n],
            recv_sem=recv_sem.at[layer * 3 + w, n],
            device_id={"dp": me + to},
            device_id_type=pl.DeviceIdType.MESH,
        )

    def piece(w, ref, p):
        return ref.at[:, pl.ds(pl.multiple_of(p * 256, 256), 256)] if w == 2 else ref.at[pl.ds(pl.multiple_of(p * 16, 16), 16)]

    def cut_copy(kind, n, p, source, target, to, w=None):
        w = n if w is None else w
        return pltpu.make_async_remote_copy(
            src_ref=piece(w, source, p),
            dst_ref=piece(w, target, p),
            send_sem=cut_send.at[kind, n, p],
            recv_sem=cut_recv.at[kind, n, p],
            device_id={"dp": me + to},
            device_id_type=pl.DeviceIdType.MESH,
        )

    def load(w, layer, slot):
        source = g[w].at[0, layer, block(w, me + away(w, slot))]
        return pltpu.make_async_copy(source, part(w, layer, slot + 4), load_sem.at[layer * 3 + w, slot])

    def swap(w, layer, slot):
        source = g[w].at[0, layer, block(w, me + other + away(w, slot))]
        if (layer, slot) == (0, 7):
            return PIECES, lambda p: cut_copy(0, w, p, source, part(w, layer, slot), other)
        return 1, lambda p: copy(w, layer, slot, source, part(w, layer, slot), other)

    def first(w, layer, slot):
        source, target, to = part(w, layer, 4 + slot), part(w, layer, 8 + slot), hop[AXES[w][0]]
        if (layer, slot) == (0, 7):
            return PIECES, lambda p: cut_copy(1, w, p, source, target, to)
        return 1, lambda p: copy(w, layer, 8 + slot - 4, source, target, to)

    def second(w, layer, slot):
        return copy(w, layer, 12 + slot - 2, part(w, layer, slot), part(w, layer, 8 + slot), hop[AXES[w][1]])

    def third(w, layer):
        source, target, to = part(w, layer, 1), part(w, layer, 9), hop[AXES[w][2]]
        if layer == LAYERS - 1:
            return PIECES, lambda p: cut_copy(2, w, p, source, target, to)
        return 1, lambda p: copy(w, layer, 14, source, target, to)

    early = [(w, layer, slot) for layer in range(LAYERS) for slot in (7, 6, 5, 4) for w in range(3)]
    late = [(w, layer, slot) for pair in ((3, 2), (1,), (0,)) for layer in range(LAYERS) for slot in pair for w in range(3)]
    barrier = pltpu.get_barrier_semaphore()
    for to in (other, *hop):
        pl.semaphore_signal(barrier, inc=1, device_id={"dp": me + to}, device_id_type=pl.DeviceIdType.MESH)
    for unit in early[:3]:
        load(*unit).start()
    pl.semaphore_wait(barrier, 4)

    swaps = [swap(*unit) for unit in early + late]
    for p in range(PIECES):
        for w in range(3):
            swaps[w][1](p).start()
    for unit in early[3:6]:
        load(*unit).start()
    for _, c in swaps[3:WINDOW]:
        c(0).start()
    for unit in early[6:]:
        load(*unit).start()

    def done(copies, side):
        n, c = copies
        if n == 1:
            getattr(c(0), side)()
        else:
            each(n, lambda p: getattr(c(p), side)())

    def add_up(sources, r, c):
        acc = sources[0][r, c].astype(F32)
        for s in sources[1:]:
            acc += s[r, c].astype(F32)
        return acc

    def total(sources, target):
        def tile(r, c):
            target[r, c] = add_up(sources, r, c).astype(BF16)

        tiles(*target.shape, tile)

    def join(w, layer, slot, p, swap_copy, first_copy):
        swap_copy.wait_recv()
        mine, theirs = part(w, layer, 4 + slot), part(w, layer, slot)
        if p is not None:
            mine, theirs = piece(w, mine, p), piece(w, theirs, p)
        total([mine, theirs], mine)
        first_copy.start()

    for w in range(3):
        load(w, 0, 7).wait()

    @functools.partial(each, PIECES)
    def _(p):
        for w in range(3):
            join(w, 0, 7, p, swaps[w][1](p), first(w, 0, 7)[1](p))

    for i, (w, layer, slot) in enumerate(early):
        if i >= 3:
            load(w, layer, slot).wait()
            join(w, layer, slot, None, swaps[i][1](0), first(w, layer, slot)[1](0))
        load(w, layer, slot - 4).start()
        if i + WINDOW < len(swaps):
            swaps[i + WINDOW][1](0).start()

    loads = [pltpu.make_async_copy(m_in[w], m[w], in_sem.at[w, 0]) for w in range(3)]
    for c in loads:
        c.start()

    def tile_load(w, layer, i, slot):
        source = v_in[w].at[layer, pl.ds(pl.multiple_of(i * 16, 16), 16)]
        return pltpu.make_async_copy(source, (tall if w == 2 else wide).at[slot], tile_sem.at[int(w == 2), slot])

    for i in range(4):
        tile_load(0, 0, i, i).start()
        tile_load(2, 0, i, i).start()

    squares[...] = jnp.zeros_like(squares)
    freed = set()
    for i, (w, layer, slot) in enumerate(late, len(early)):
        if layer not in freed:
            freed.add(layer)
            for x in range(3):
                for sent_slot in (7, 6, 5):
                    done(first(x, layer, sent_slot), "wait_send")
                for axis in (1, 2):
                    to = {"dp": me + hop[AXES[x][axis]]}
                    pl.semaphore_signal(free_sem.at[layer * 3 + x, axis - 1], inc=1, device_id=to, device_id_type=pl.DeviceIdType.MESH)
        load(w, layer, slot).wait()
        done(swaps[i], "wait_recv")
        done(first(w, layer, slot + 4), "wait_recv")
        sources = [part(w, layer, slot + 4), part(w, layer, slot), part(w, layer, 12 + slot)]
        if slot < 2:
            second(w, layer, slot + 2).wait_recv()
            sources.append(part(w, layer, 10 + slot))
        if slot == 0:

            def tile(r, c, sources=sources, w=w, layer=layer):
                v[w][layer, r, c] = add_up(sources, r, c)

            tiles(rows[w], columns[w], tile)
        elif slot == 1:
            pl.semaphore_wait(free_sem.at[layer * 3 + w, 1], 1)
            n, c = third(w, layer)
            target = part(w, layer, slot)
            if n == 1:
                total(sources, target)
                c(0).start()
            else:

                @functools.partial(each, n)
                def _(p, w=w, c=c, sources=sources, target=target):
                    total([piece(w, ref, p) for ref in sources], piece(w, target, p))
                    c(p).start()

        else:
            total(sources, part(w, layer, slot))
            if slot == 3:
                pl.semaphore_wait(free_sem.at[layer * 3 + w, 0], 1)
            second(w, layer, slot).start()
        if i + WINDOW < len(swaps):
            swaps[i + WINDOW][1](0).start()

    def finish(w, last, grad):
        def tile(r, c):
            rounded = (grad[r, c] + last[r, c].astype(F32)).astype(BF16).astype(F32)
            grad[r, c] = rounded
            squares[:, : c.size] += rounded * rounded

        tiles(*last.shape, tile)

    squares[...] = jnp.zeros_like(squares)
    for w in range(3):
        done(third(w, 0), "wait_recv")
        finish(w, part(w, 0, 9), v[w].at[0])

    for copies in swaps:
        done(copies, "wait_send")
    for layer, w in UNITS:
        done(first(w, layer, 4), "wait_send")
        for slot in (3, 2):
            second(w, layer, slot).wait_send()
    for w in range(3):
        done(third(w, 0), "wait_send")

    @functools.partial(each, PIECES)
    def _(p):
        for w in range(3):
            third(w, 1)[1](p).wait_recv()
            finish(w, piece(w, part(w, 1, 9), p), piece(w, v[w].at[1], p))

    for w in range(3):
        done(third(w, 1), "wait_send")

    everyone = [
        pltpu.make_async_remote_copy(
            src_ref=all_squares.at[0],
            dst_ref=all_squares.at[k],
            send_sem=sum_send.at[k],
            recv_sem=sum_recv.at[k],
            device_id={"dp": lax.rem(me + k, DEVICES)},
            device_id_type=pl.DeviceIdType.MESH,
        )
        for k in range(1, DEVICES)
    ]
    s = squares[:8] + squares[8:]
    all_squares[0] = sum(s[:, c : c + 128] for c in range(0, WIDTH, 128))
    for c in everyone:
        c.start()
    loads += [pltpu.make_async_copy(wt[w].at[:, block(w, me)], out[w].at[:, block(w, me)], in_sem.at[w, 1]) for w in range(3)]
    for c in loads[3:]:
        c.start()
    for c in loads:
        c.wait()
    for c in everyone:
        c.wait_recv()
    s = jnp.sum(jnp.sum(jnp.sum(all_squares[...], axis=0), axis=0, keepdims=True), axis=1, keepdims=True)
    factor = jnp.minimum(1.0, 0.5 * lax.rsqrt(s / count + 1e-30))

    def forward(w, layer, k, bit):
        where = out[w].at[layer, block(w, me + away(w, k))]
        return copy(w, layer, 7 + k if bit == 3 else (k | 1 << bit) - 1, where, where, other if bit == 3 else hop[AXES[w][2 - bit]])

    def forward_cut(bit, p):
        where = out[0].at[0, block(0, me)]
        return cut_copy(5, bit, p, where, where, hop[AXES[0][2 - bit]], 0)

    def arrived_cut(k, p):
        source, target = out[0].at[0, block(0, me)], out[0].at[0, block(0, me + away(0, k))]
        bit = k.bit_length() - 1
        return cut_copy(5, bit, p, source, target, hop[AXES[0][2 - bit]], 0)

    def head(w):
        return head_rows(rows[w])

    def rest(w, k, p):
        lo = head(w)
        where = out[w].at[0, block(w, me + away(w, k))]
        return where.at[pl.ds(lo, rows[w] - lo), pl.ds(pl.multiple_of(p * (columns[w] // 2), 128), columns[w] // 2)]

    def rest_copy(w, k, p):
        return pltpu.make_async_remote_copy(
            src_ref=rest(w, k, p),
            dst_ref=rest(w, k, p),
            send_sem=cut_send.at[3 if k == 3 else 4, w, p],
            recv_sem=cut_recv.at[3 if k == 3 else 4, w, p],
            device_id={"dp": me + (hop[AXES[w][0]] if k == 3 else other)},
            device_id_type=pl.DeviceIdType.MESH,
        )

    def rest_arrived(w, k, p, to):
        where = rest(w, k, p) if to is None else to
        kind = 3 if to is None else 4
        return pltpu.make_async_remote_copy(
            src_ref=where,
            dst_ref=where,
            send_sem=cut_send.at[kind, w, p],
            recv_sem=cut_recv.at[kind, w, p],
            device_id={"dp": me + other},
            device_id_type=pl.DeviceIdType.MESH,
        )

    def tail_copy(w, layer):
        source = out[w].at[layer, block(w, me + away(w, 3))]
        if layer == 1:
            return pltpu.make_async_copy(source, tail[w].at[: rows[w]], in_sem.at[w, 0])
        return pltpu.make_async_copy(source.at[: head(w)], tail[w].at[rows[w] :], in_sem.at[w, 1])

    def arrived(w, layer, k):
        bit = k.bit_length() - 1
        return copy(w, layer, k - 1, out[w].at[layer, block(w, me)], out[w].at[layer, block(w, me + away(w, k))], hop[AXES[w][2 - bit]])

    sent = []

    def pass_on(w, layer, k):
        for bit in range(4):
            if not k >> bit or bit == 3:
                sent.append(forward(w, layer, k, bit))
                sent[-1].start()

    def advance(w, layer, i):
        slot = i if w < 2 else lax.rem(layer * (rows[w] // 16) + i, 4)
        tile_load(w, layer, i, slot).wait()
        r = pl.ds(pl.multiple_of(i * 16, 16), 16)
        at = pl.ds(pl.multiple_of(me * rows[w] + i * 16, 16), 16)
        for column in range(0, columns[w], 256):
            c = pl.ds(column, 256)
            old = (tall if w == 2 else wide)[slot, :, c]
            new, m[w][layer, r, c], v[w][layer, r, c] = adamw(
                out[w][layer, at, c].astype(F32), m[w][layer, r, c], old, v[w][layer, r, c] * factor
            )
            out[w][layer, at, c] = new
        if w == 0:
            tile_load(1, layer, i, slot).start()
        elif w == 1 and layer + 1 < LAYERS:
            tile_load(0, layer + 1, i, slot).start()
        elif w == 2:
            ahead = i + 4

            @pl.when(ahead < rows[w] // 16)
            def _():
                tile_load(w, layer, ahead, slot).start()

            if layer + 1 < LAYERS:

                @pl.when(ahead >= rows[w] // 16)
                def _():
                    tile_load(w, layer + 1, ahead - rows[w] // 16, slot).start()

    for layer, w in UNITS:
        if (layer, w) == (0, 0):

            @functools.partial(each, PIECES)
            def _(p):
                advance(0, 0, p)
                for bit in range(3):
                    forward_cut(bit, p).start()

            sent.append(forward(w, layer, 0, 3))
            sent[-1].start()
        else:
            lax.fori_loop(0, rows[w] // 16, lambda i, _, w=w, layer=layer: advance(w, layer, i), None)
            pass_on(w, layer, 0)
    order = gather_order()
    last = [(0, w, 7) for w in range(3)]
    assert sorted(order[-3:]) == last
    for layer, w, k in order[:-3]:
        if (layer, w) == (0, 0) and k & k - 1 == 0:
            each(PIECES, lambda p, k=k: arrived_cut(k, p).wait_recv())
        else:
            arrived(w, layer, k).wait_recv()
        if k == 3:
            if layer == 0:
                each(2, lambda p, w=w: rest_copy(w, 3, p).start())
            tail_copy(w, layer).start()
            sent.append(forward(w, layer, k, 3))
            sent[-1].start()
        else:
            pass_on(w, layer, k)

    @functools.partial(each, 2)
    def _(p):
        for w in range(3):
            rest_arrived(w, 7, p, None).wait_recv()
            rest_copy(w, 7, p).start()

    for layer, w in UNITS:
        for k in range(7):
            where = out[w].at[layer, block(w, me + other + away(w, k))]
            copy(w, layer, 7 + k, where, where, other).wait_recv()
    for c in sent:
        c.wait_send()
    for c in everyone:
        c.wait_send()
    for bit in range(3):
        each(PIECES, lambda p, bit=bit: forward_cut(bit, p).wait_send())
    for w in range(3):
        for layer in range(LAYERS):
            tail_copy(w, layer).wait()

    def theirs(w, p):
        lo = head(w)
        where = out[w].at[0, block(w, me + other + away(w, 7))]
        return where.at[pl.ds(lo, rows[w] - lo), pl.ds(pl.multiple_of(p * (columns[w] // 2), 128), columns[w] // 2)]

    @functools.partial(each, 2)
    def _(p):
        for w in range(3):
            rest_arrived(w, 7, p, theirs(w, p)).wait_recv()
            rest_copy(w, 3, p).wait_send()
            rest_copy(w, 7, p).wait_send()


def write_kernel(n, *refs):
    sem = refs[2 * n]
    copies = [pltpu.make_async_copy(refs[i].at[layer], refs[n + i].at[layer], sem.at[i, layer]) for i in range(n) for layer in range(LAYERS)]
    for c in copies:
        c.start()
    for c in copies:
        c.wait()


def write(new, held):
    n = len(new)
    size = sum(one.size * one.dtype.itemsize for one in new)
    return pl.pallas_call(
        functools.partial(write_kernel, n),
        out_shape=[jax.ShapeDtypeStruct(one.shape, one.dtype) for one in new],
        in_specs=[pl.BlockSpec(memory_space=pltpu.VMEM)] * n,
        out_specs=[pl.BlockSpec(memory_space=pltpu.HBM)] * n,
        scratch_shapes=[pltpu.SemaphoreType.DMA((n, LAYERS))],
        compiler_params=pltpu.CompilerParams(vmem_limit_bytes=VMEM - held - SLACK),
        cost_estimate=pl.CostEstimate(flops=size * 4, bytes_accessed=size, transcendentals=0),
        name="write",
    )(*(pltpu.with_memory_space_constraint(a, pltpu.VMEM) for a in new))


def tail_kernel(blocks, staged, *refs):
    tails, out, sem = refs[:3], refs[6:9], refs[9]
    me = lax.axis_index("dp")
    far = 14 - 2 * (me // 2)
    at = far + (lax.rem(me, 2) if staged else 1 - lax.rem(me, 2))
    loads = []
    if staged:
        loads = [pltpu.make_async_copy(refs[i], refs[11 + i], refs[10].at[i]) for i in range(3)]
        tails = refs[11:14]
        for c in loads:
            c.start()
    copies = []
    for i, source in enumerate(tails):
        n = blocks[i]
        if loads:
            loads[i].wait()
        for layer, (lo, size) in ((1, (0, n)), (0, (n, source.shape[0] - n))):
            target = out[i].at[layer, pl.ds(pl.multiple_of(at * n, 16), size)]
            copies.append(pltpu.make_async_copy(source.at[lo : lo + size], target, sem.at[i, layer]))
            copies[-1].start()
    for c in copies:
        c.wait()


def put(tails, whole, staged):
    hbm, vmem = pl.BlockSpec(memory_space=pltpu.HBM), pl.BlockSpec(memory_space=pltpu.VMEM)
    space, dma = (pltpu.HBM if staged else pltpu.VMEM), pltpu.SemaphoreType.DMA
    size = sum(t.size for t in tails)
    return pl.pallas_call(
        functools.partial(tail_kernel, [one.shape[1] // DEVICES for one in whole], staged),
        out_shape=[jax.ShapeDtypeStruct(one.shape, one.dtype) for one in whole],
        in_specs=[hbm if staged else vmem] * 3 + [hbm] * 3,
        out_specs=[hbm] * 3,
        input_output_aliases={3: 0, 4: 1, 5: 2},
        scratch_shapes=[dma((3, LAYERS)), dma((3,))] + [pltpu.VMEM(t.shape, BF16) for t in tails if staged],
        compiler_params=pltpu.CompilerParams(vmem_limit_bytes=6 * 2**20),
        cost_estimate=pl.CostEstimate(flops=size * 8, bytes_accessed=size * 4, transcendentals=0),
        name="put",
    )(*(pltpu.with_memory_space_constraint(t, space) for t in tails), *whole)


def solution(mesh):
    def step(*arrays):
        weights, moments = arrays[3:6], arrays[6:12]
        blocks = [one.shape for one in moments[:3]]
        new = [pltpu.VMEM(w.shape, BF16) for w in weights] + [pltpu.VMEM(one.shape, F32) for one in moments]
        new += [pltpu.HBM((b[1] + head_rows(b[1]), b[2]), BF16) for b in blocks]
        held = sum(one.size * one.dtype.itemsize for one in (*weights, *moments))
        hbm, vmem = pl.BlockSpec(memory_space=pltpu.HBM), pl.BlockSpec(memory_space=pltpu.VMEM)
        dma = pltpu.SemaphoreType.DMA
        count = float(sum(w.size for w in weights))
        new = pl.pallas_call(
            functools.partial(step_kernel, count),
            out_shape=new,
            in_specs=[hbm] * 12,
            out_specs=[vmem] * 9 + [hbm] * 3,
            scratch_shapes=[
                pltpu.VMEM((4, 16, blocks[0][2]), F32),
                pltpu.VMEM((4, 16, blocks[2][2]), F32),
                pltpu.VMEM((16, WIDTH), F32),
                pltpu.VMEM((DEVICES, 8, 128), F32),
                dma((6, 15)),
                dma((6, 15)),
                dma((6, 8)),
                dma((3, 2)),
                dma((2, 4)),
                dma((DEVICES,)),
                dma((DEVICES,)),
                pltpu.SemaphoreType.REGULAR((6, 2)),
                dma((6, 3, PIECES)),
                dma((6, 3, PIECES)),
            ],
            compiler_params=pltpu.CompilerParams(collective_id=0, has_side_effects=True, vmem_limit_bytes=VMEM - held - SLACK),
            name="step",
        )(*(pltpu.with_memory_space_constraint(a, pltpu.HBM) for a in arrays))
        new, tails = new[:9], new[9:]
        mine = [lax.ppermute(t, "dp", [(i, i ^ (8, 4, 2)[AXES[w][0]]) for i in range(DEVICES)]) for w, t in enumerate(tails)]
        gate, up, down, *moments = write(new, held)
        *mine, gate = lax.optimization_barrier((*mine, gate))
        theirs = [lax.ppermute(t, "dp", [(i, i ^ 1) for i in range(DEVICES)]) for t in mine]
        whole = put(theirs, put(mine, [gate, up, down], True), False)
        return (*whole, *moments)

    all_of, cut = P(None, None, None), P(None, "dp", None)
    return jax.shard_map(
        step,
        mesh=mesh,
        in_specs=(P(("rep", "dp"), None, None, None),) * 3 + (all_of,) * 3 + (cut,) * 6,
        out_specs=(P("rep", None, None),) * 3 + (P("rep", "dp", None),) * 6,
        check_vma=False,
    )
```
